32 devices in a mesh: ctx: 4 (over z), shard: 4 (over y, x), dp: 2 (over core).
Axes of the slice: x: 2, y: 2, z: 4, core: 2. Of those that a mesh axis runs over, the one named last changes fastest.
Arguments:
- tokens: bfloat16 [6, 1024, 2048], P('dp', 'ctx'), may hold values from -6 to 6
- gain_attn: float32 [2048], replicated, may hold values from 0.5 to 1.5
- gain_mlp: float32 [2048], replicated, may hold values from 0.5 to 1.5
- gain_query: float32 [128], replicated, may hold values from 0.5 to 1.5
- key_norm_gain: float32 [128], replicated, may hold values from 0.5 to 1.5
- w_query: bfloat16 [2048, 4096], P(('ctx', 'dp'), 'shard'), may hold values from -0.125 to 0.125
- key_matrix: bfloat16 [2048, 512], P(('ctx', 'dp'), 'shard'), may hold values from -0.125 to 0.125
- value_matrix: bfloat16 [2048, 512], P(('ctx', 'dp'), 'shard'), may hold values from -0.125 to 0.125
- w_out: bfloat16 [2048, 4096], P(('ctx', 'dp'), 'shard'), may hold values from -1.5 to 1.5
- w_gate: bfloat16 [4, 2048, 768], P('shard', ('ctx', 'dp')), may hold values from -0.125 to 0.125
- w_up: bfloat16 [4, 2048, 768], P('shard', ('ctx', 'dp')), may hold values from -0.125 to 0.125
- w_down: bfloat16 [4, 2048, 768], P('shard', ('ctx', 'dp')), may hold values from -0.21875 to 0.21875
- expert_ids: int32 [6, 1024, 2], P('dp', ('ctx', 'shard')), may hold values from 0 to 3, all different within a row; in each aligned block of 64 rows (0 to 63, 64 to 127, ..., all dimensions but the last counted through in order) at most 48 rows name the same one
- route_weight: float32 [6, 1024, 2], P('dp', ('ctx', 'shard')), may hold values from 0.2 to 1
- cotangent: bfloat16 [6, 1024, 2048], P('dp', ('ctx', 'shard')), may hold values from -6 to 6
Outputs:
- block_out: bfloat16 [6, 1024, 2048], P('dp', ('ctx', 'shard'))
- grad_tokens: float32 [6, 1024, 2048], P('dp', ('ctx', 'shard'))
- softmax_lse: float32 [6, 32, 1024], P('dp', 'shard', 'ctx')
- route_grad: float32 [6, 1024, 2], P('dp', ('ctx', 'shard'))
- grad_gain_attn: float32 [2048], replicated
- grad_gain_mlp: float32 [2048], replicated
- grad_gain_query: float32 [128], replicated
- grad_gain_key: float32 [128], replicated
- grad_w_query: float32 [2048, 4096], P(('ctx', 'dp'), 'shard')
- grad_w_key: float32 [2048, 512], P(('ctx', 'dp'), 'shard')
- grad_w_value: float32 [2048, 512], P(('ctx', 'dp'), 'shard')
- grad_w_out: float32 [2048, 4096], P(('ctx', 'dp'), 'shard')
- grad_w_gate: float32 [4, 2048, 768], P('shard', ('ctx', 'dp'))
- grad_w_up: float32 [4, 2048, 768], P('shard', ('ctx', 'dp'))
- grad_w_down: float32 [4, 2048, 768], P('shard', ('ctx', 'dp'))
The draws below stay inside these ranges and needn't reach their ends.
Inputs may be any that keep to these rules, and one draw needn't show every extreme that they name: `expert_ids`: each row names 2 different experts. In each aligned block of 64 rows (all leading dimensions taken in order) no expert is named by more than 48 rows, and in some block one expert is named by exactly 48 rows.
All inputs are finite; a program needn't handle non-finite values.
Results may differ from the reference program's by a relative error of at most 0.02.
Values may be sent and summed in bfloat16 or wider, within the bound.
A program may use at most 192 MiB of HBM per device.

```python
import math
import jax
import jax.numpy as jnp
import numpy as np
from jax import lax

MODEL_DIM = 2048
QUERY_HEADS = 32
KEY_VALUE_HEADS = 4
HEAD_SIZE = 128
EXPERT_HIDDEN = 768
TOPW = 2
BLK = 128
EXPERT_COUNT = 4
SEQUENCE_LENGTH = 1024
NSEQ = 6
ROWS_DEV = 64
MOST = 48
N_CTX = 4


def levels(stream_key, dims, pieces, low, largest):
    def one(axis_at, blocks):
        heights = jax.random.uniform(jax.random.fold_in(jax.random.fold_in(stream_key, 6), axis_at), (blocks,), jnp.float32, low / len(pieces), largest / len(pieces))
        return jnp.repeat(jnp.exp(heights), dims[axis_at] // blocks).reshape((-1,) + (1,) * (len(dims) - axis_at - 1))

    factor_of = one(*pieces[0])
    for cut in pieces[1:]:
        factor_of = factor_of * one(*cut)
    return factor_of


def deal_out(stream_key, own, number, rows, amount, top, reach, skew):
    ranking = jax.random.permutation(stream_key, amount)
    crowded, common = shares(amount, rows * top, reach, skew, True), shares(amount, rows * top, reach, skew, False)
    places = jnp.arange(amount)

    def named(lengths, turn):
        used = int((lengths > 0).sum())
        fixed = max(1, used // 4)
        shifted = fixed + (places - fixed + turn * (used - fixed)) % max(1, amount - fixed)
        return jnp.zeros((amount,), jnp.int32).at[ranking[jnp.where(places < fixed, places, shifted)]].set(jnp.asarray(lengths, jnp.int32))

    lengths = jnp.where(number % 4 == 0, named(crowded, number // 4), named(common, number - number // 4 - 1))
    mixed = jax.random.permutation(jax.random.fold_in(own, 3), amount)
    source_of, taker = mixed[0:amount // 2 * 2:2], mixed[1:amount // 2 * 2:2]
    slack = jnp.minimum(lengths[source_of] - 1, reach - lengths[taker]) // 2
    slack = jnp.where((source_of == ranking[0]) | (taker == ranking[0]) | (lengths[taker] == 0), 0, jnp.maximum(slack, 0))
    shifted = jax.random.randint(jax.random.fold_in(own, 4), (amount // 2,), 0, 1 << 20) % (slack + 1)
    lengths = lengths.at[source_of].add(-shifted).at[taker].add(shifted)
    members = jnp.searchsorted(jnp.cumsum(lengths), jnp.arange(rows * top), side="right").astype(jnp.int32)
    table = members.reshape(top, rows).T
    table = table[jax.random.permutation(jax.random.fold_in(own, 1), rows)]
    turn = jax.random.randint(jax.random.fold_in(own, 2), (rows, 1), 0, top)
    return jnp.take_along_axis(table, (jnp.arange(top)[None, :] + turn) % top, axis=1)


def shares(number_of, total, limit, slope, full):
    loads = [(1 << 20) // math.isqrt(grade ** slope) + 1 for grade in range(1, number_of + 1)]
    largest = limit if full else min(limit, max(-(-total // number_of), total * loads[0] // sum(loads)))
    least = 1 if total - largest >= number_of - 1 else 0
    counts, rest = [largest] + [least] * (number_of - 1), total - largest - least * (number_of - 1)
    while rest > 0:
        free = [i for i in range(1, number_of) if counts[i] < largest] or [i for i in range(1, number_of) if counts[i] < limit]
        whole, left = sum([loads[i] for i in free]), rest
        for i in free:
            extra = min(limit - counts[i], max(1, left * loads[i] // whole), rest)
            counts[i] = counts[i] + extra
            rest = rest - extra
    return np.array(counts)


def bell_draw(stream_key, shape, width, bound, cuts=(), kind=jnp.bfloat16):
    result = jax.random.normal(stream_key, shape, jnp.float32) * width
    if len(cuts) > 0:
        result = levels(stream_key, shape, cuts, -0.22, 0.18) * result
    return jnp.clip(result, min=-bound, max=bound).astype(kind)


def setup_inputs(seed: int = 0) -> dict:
    key_of = jax.random.split(jax.random.key(seed), 16)
    tokens = bell_draw(key_of[0], (NSEQ, SEQUENCE_LENGTH, MODEL_DIM), 1.0, 6.0, ((0, 2), (1, 4)))
    gain_attn = jnp.clip(1.0 + 0.1 * jax.random.normal(key_of[1], (MODEL_DIM,), jnp.float32), 0.5, 1.5)
    gain_mlp = jnp.clip(1.0 + 0.1 * jax.random.normal(key_of[2], (MODEL_DIM,), jnp.float32), 0.5, 1.5)
    gain_query = jnp.clip(1.0 + 0.1 * jax.random.normal(key_of[3], (HEAD_SIZE,), jnp.float32), 0.5, 1.5)
    key_norm_gain = jnp.clip(1.0 + 0.1 * jax.random.normal(key_of[4], (HEAD_SIZE,), jnp.float32), 0.5, 1.5)
    w_query = bell_draw(key_of[5], (MODEL_DIM, QUERY_HEADS * HEAD_SIZE), MODEL_DIM ** -0.5, 0.125, ((0, 8), (1, 4)))
    key_matrix = bell_draw(key_of[6], (MODEL_DIM, KEY_VALUE_HEADS * HEAD_SIZE), MODEL_DIM ** -0.5, 0.125, ((0, 8), (1, 4)))
    value_matrix = bell_draw(key_of[7], (MODEL_DIM, KEY_VALUE_HEADS * HEAD_SIZE), MODEL_DIM ** -0.5, 0.125, ((0, 8), (1, 4)))
    w_out = bell_draw(key_of[8], (MODEL_DIM, QUERY_HEADS * HEAD_SIZE), (max(8, QUERY_HEADS * HEAD_SIZE // 256)) ** -0.5, 1.5, ((0, 8), (1, 4)))
    w_gate = bell_draw(key_of[9], (EXPERT_COUNT, MODEL_DIM, EXPERT_HIDDEN), MODEL_DIM ** -0.5, 0.125, ((0, 4), (1, 8)))
    w_up = bell_draw(key_of[10], (EXPERT_COUNT, MODEL_DIM, EXPERT_HIDDEN), MODEL_DIM ** -0.5, 0.125, ((0, 4), (1, 8)))
    w_down = bell_draw(key_of[11], (EXPERT_COUNT, MODEL_DIM, EXPERT_HIDDEN), EXPERT_HIDDEN ** -0.5, 0.21875, ((0, 4), (1, 8)))
    expert_ids_keys = jax.random.split(jax.random.fold_in(key_of[12], 1), NSEQ * SEQUENCE_LENGTH // ROWS_DEV)
    expert_ids_turns = jax.random.permutation(jax.random.fold_in(key_of[12], 3), NSEQ * SEQUENCE_LENGTH // ROWS_DEV)
    expert_ids = jax.vmap(lambda own, number: deal_out(jax.random.fold_in(key_of[12], 2), own, number, ROWS_DEV, EXPERT_COUNT, TOPW, MOST, 1))(expert_ids_keys, expert_ids_turns).reshape((NSEQ, SEQUENCE_LENGTH, TOPW))
    route_weight = jnp.clip(0.2 + 0.8 * jax.random.uniform(key_of[13], (NSEQ, SEQUENCE_LENGTH, TOPW), jnp.float32) ** levels(key_of[13], (NSEQ, SEQUENCE_LENGTH, TOPW), ((0, 2), (1, 16)), -0.2, 0.2), 0.2, 1.0)
    cotangent = bell_draw(key_of[14], (NSEQ, SEQUENCE_LENGTH, MODEL_DIM), 1.0, 6.0, ((0, 2), (1, 16)))
    return dict(tokens=tokens, gain_attn=gain_attn, gain_mlp=gain_mlp, gain_query=gain_query, key_norm_gain=key_norm_gain, w_query=w_query, key_matrix=key_matrix, value_matrix=value_matrix, w_out=w_out, w_gate=w_gate, w_up=w_up, w_down=w_down, expert_ids=expert_ids, route_weight=route_weight, cotangent=cotangent)


epsilon = 1e-06
theta_base = 1000000.0
block_rows_max = 512

def folded_positions(rows, count_ctx, half_block):
    block = rows // half_block
    offset = rows % half_block
    device = block // 2
    placed = jnp.where(block % 2 == 0, device, 2 * count_ctx - 1 - device)
    return (placed * half_block + offset).astype(jnp.int32)

def rope_tables(positions, head_dim):
    freq = jnp.arange(head_dim // 2, dtype=jnp.float32) * (2.0 / head_dim)
    inverse = jnp.power(jnp.float32(theta_base), -freq)
    angles = positions.astype(jnp.float32)[:, None] * inverse[None, :]
    return (jnp.cos(angles), jnp.sin(angles))

def rotate(field, cosine, sine):
    half = field.shape[-1] // 2
    first = field[..., :half]
    second = field[..., half:]
    cos_b = cosine[:, None, :]
    sin_b = sine[:, None, :]
    return jnp.concatenate([first * cos_b - second * sin_b, second * cos_b + first * sin_b], -1)

def rotate_back(grad, cosine, sine):
    half = grad.shape[-1] // 2
    first = grad[..., :half]
    second = grad[..., half:]
    cos_b = cosine[:, None, :]
    sin_b = sine[:, None, :]
    return jnp.concatenate([first * cos_b + second * sin_b, second * cos_b - first * sin_b], -1)

def inv_rms(field):
    return lax.rsqrt(lax.optimization_barrier(jnp.mean(field * field, -1, keepdims=True)) + epsilon)

def norm_backward_step(grad_normed, normed_hat, inverse, gain):
    scaled = grad_normed * gain
    return inverse * (scaled - normed_hat * lax.optimization_barrier(jnp.mean(scaled * normed_hat, -1, keepdims=True)))

def head_forward(queries, keys, values, positions):
    rows = queries.shape[0]
    query_group = queries.shape[1]
    size = min(block_rows_max, rows)
    count = rows // size
    query_blocks = queries.reshape(count, size, query_group, HEAD_SIZE)
    pos_blocks = positions.reshape(count, size)

    def one_block(inputs):
        query_part, pos_part = inputs
        scores = jnp.einsum('qgd,kd->gqk', query_part.astype(jnp.float32), keys.astype(jnp.float32)) * HEAD_SIZE ** (-0.5)
        visible = pos_part[:, None] >= positions[None, :]
        scores = jnp.where(visible[None], scores, -1e+30)
        top_val = lax.optimization_barrier(jnp.max(scores, -1, keepdims=True))
        log_total = top_val[..., 0] + jnp.log(lax.optimization_barrier(jnp.sum(jnp.exp(scores - top_val), -1)))
        probs = jnp.where(visible[None], jnp.exp(scores - log_total[..., None]), 0.0).astype(jnp.bfloat16)
        output = jnp.einsum('gqk,kd->qgd', probs.astype(jnp.float32), values.astype(jnp.float32))
        return (output, log_total)
    output, log_total = lax.map(one_block, (query_blocks, pos_blocks))
    return (output.reshape(rows, query_group, HEAD_SIZE), log_total.transpose(1, 0, 2).reshape(query_group, rows))

def head_backward(queries, keys, values, positions, log_total, attention_gradient, attn_heads):
    rows = queries.shape[0]
    query_group = queries.shape[1]
    size = min(block_rows_max, rows)
    count = rows // size
    query_blocks = queries.reshape(count, size, query_group, HEAD_SIZE)
    pos_blocks = positions.reshape(count, size)
    lse_blocks = log_total.reshape(query_group, count, size).transpose(1, 0, 2)
    grad_blocks = attention_gradient.reshape(count, size, query_group, HEAD_SIZE)
    attn_blocks = attn_heads.reshape(count, size, query_group, HEAD_SIZE)

    def one_block(state_pair, inputs):
        grad_keys, value_gradients = state_pair
        query_part, pos_part, lse_part, grad_part, attn_part = inputs
        scores = jnp.einsum('qgd,kd->gqk', query_part.astype(jnp.float32), keys.astype(jnp.float32)) * HEAD_SIZE ** (-0.5)
        visible = pos_part[:, None] >= positions[None, :]
        scores = jnp.where(visible[None], scores, -1e+30)
        probs = jnp.where(visible[None], jnp.exp(scores - lse_part[..., None]), 0.0)
        probs_bf = probs.astype(jnp.bfloat16)
        delta = lax.optimization_barrier(jnp.sum(grad_part.astype(jnp.float32) * attn_part.astype(jnp.float32), -1))
        grad_probs = jnp.einsum('qgd,kd->gqk', grad_part.astype(jnp.float32), values.astype(jnp.float32))
        grad_scores = (probs * (grad_probs - delta.T[..., None]) * HEAD_SIZE ** (-0.5)).astype(jnp.bfloat16)
        grad_query = jnp.einsum('gqk,kd->qgd', grad_scores.astype(jnp.float32), keys.astype(jnp.float32))
        grad_keys = grad_keys + jnp.einsum('gqk,qgd->kd', grad_scores.astype(jnp.float32), query_part.astype(jnp.float32))
        value_gradients = value_gradients + jnp.einsum('gqk,qgd->kd', probs_bf.astype(jnp.float32), grad_part.astype(jnp.float32))
        return ((grad_keys, value_gradients), grad_query)
    offset_begin = (jnp.zeros((rows, HEAD_SIZE), jnp.float32), jnp.zeros((rows, HEAD_SIZE), jnp.float32))
    (grad_keys, value_gradients), grad_query = lax.scan(one_block, offset_begin, (query_blocks, pos_blocks, lse_blocks, grad_blocks, attn_blocks))
    return (grad_query.reshape(rows, query_group, HEAD_SIZE), grad_keys, value_gradients)

def reference(tokens, gain_attn, gain_mlp, gain_query, key_norm_gain, w_query, key_matrix, value_matrix, w_out, w_gate, w_up, w_down, expert_ids, route_weight, cotangent):
    query_group = QUERY_HEADS // KEY_VALUE_HEADS
    positions = folded_positions(jnp.arange(SEQUENCE_LENGTH), N_CTX, BLK)
    cosine, sine = rope_tables(positions, HEAD_SIZE)

    def one_sequence(totals, inputs):
        token_rows, ids_rows, weight_rows, cot_rows = inputs
        residual_rows = token_rows.astype(jnp.float32)
        inverse_one = inv_rms(residual_rows)
        hat_one = residual_rows * inverse_one
        first_normalized = (hat_one * gain_attn).astype(jnp.bfloat16)
        queries = jnp.dot(first_normalized, w_query, preferred_element_type=jnp.float32).reshape(SEQUENCE_LENGTH, QUERY_HEADS, HEAD_SIZE)
        keys_before_norm = jnp.dot(first_normalized, key_matrix, preferred_element_type=jnp.float32).reshape(SEQUENCE_LENGTH, KEY_VALUE_HEADS, HEAD_SIZE)
        values_projected = jnp.dot(first_normalized, value_matrix, preferred_element_type=jnp.float32).reshape(SEQUENCE_LENGTH, KEY_VALUE_HEADS, HEAD_SIZE)
        inverse_q = inv_rms(queries)
        hat_q = queries * inverse_q
        key_inverse_radius = inv_rms(keys_before_norm)
        key_unit_rows = keys_before_norm * key_inverse_radius
        query_rows_half = rotate(hat_q * gain_query, cosine, sine).astype(jnp.bfloat16)
        keys_bf = rotate(key_unit_rows * key_norm_gain, cosine, sine).astype(jnp.bfloat16)
        values_bf = values_projected.astype(jnp.bfloat16)
        group_rows = query_rows_half.reshape(SEQUENCE_LENGTH, KEY_VALUE_HEADS, query_group, HEAD_SIZE).transpose(1, 0, 2, 3)
        keys_heads = keys_bf.transpose(1, 0, 2)
        values_heads = values_bf.transpose(1, 0, 2)
        heads_out, heads_lse = lax.map(lambda a: head_forward(a[0], a[1], a[2], positions), (group_rows, keys_heads, values_heads))
        attention_half_precision = heads_out.transpose(1, 0, 2, 3).reshape(SEQUENCE_LENGTH, QUERY_HEADS * HEAD_SIZE).astype(jnp.bfloat16)
        logsumexp_rows = heads_lse.reshape(QUERY_HEADS, SEQUENCE_LENGTH)
        hidden = residual_rows + jnp.dot(attention_half_precision, w_out.T, preferred_element_type=jnp.float32)
        inverse_two = inv_rms(hidden)
        hat_two = hidden * inverse_two
        normed_two = (hat_two * gain_mlp).astype(jnp.bfloat16)

        def expert_forward(weights):
            gate_w, up_w, down_w = weights
            gate_pre = jnp.dot(normed_two, gate_w, preferred_element_type=jnp.float32)
            up_pre = jnp.dot(normed_two, up_w, preferred_element_type=jnp.float32)
            inner_bf = (jax.nn.silu(gate_pre) * up_pre).astype(jnp.bfloat16)
            return jnp.dot(inner_bf, down_w.T, preferred_element_type=jnp.float32).astype(jnp.bfloat16)
        expert_out = lax.map(expert_forward, (w_gate, w_up, w_down))
        onehot = (ids_rows[:, :, None] == jnp.arange(EXPERT_COUNT, dtype=jnp.int32)[None, None, :]).astype(jnp.float32)
        coefs = jnp.einsum('tk,tke->et', weight_rows, onehot)
        mixture = jnp.einsum('et,etd->td', coefs, expert_out.astype(jnp.float32))
        block_out = (hidden + mixture).astype(jnp.bfloat16)
        grad_top = cot_rows.astype(jnp.float32)
        per_expert = jnp.einsum('td,etd->et', grad_top, expert_out.astype(jnp.float32))
        route_grad = jnp.einsum('tke,et->tk', onehot, per_expert)

        def expert_backward(total, weights):
            gate_w, up_w, down_w, coef_col = weights
            gate_pre = jnp.dot(normed_two, gate_w, preferred_element_type=jnp.float32)
            up_pre = jnp.dot(normed_two, up_w, preferred_element_type=jnp.float32)
            inner_bf = (jax.nn.silu(gate_pre) * up_pre).astype(jnp.bfloat16)
            gate_sig = jax.nn.sigmoid(gate_pre)
            gate_act = gate_pre * gate_sig
            grad_rows = (coef_col[:, None] * grad_top).astype(jnp.bfloat16)
            grad_inner = jnp.dot(grad_rows, down_w, preferred_element_type=jnp.float32)
            grad_gate = (grad_inner * up_pre * gate_sig * (1.0 + gate_pre * (1.0 - gate_sig))).astype(jnp.bfloat16)
            grad_up = (grad_inner * gate_act).astype(jnp.bfloat16)
            grad_down_w = jnp.dot(grad_rows.T, inner_bf, preferred_element_type=jnp.float32)
            grad_gate_w = jnp.dot(normed_two.T, grad_gate, preferred_element_type=jnp.float32)
            grad_up_w = jnp.dot(normed_two.T, grad_up, preferred_element_type=jnp.float32)
            grad_slot = (jnp.dot(grad_gate, gate_w.T, preferred_element_type=jnp.float32) + jnp.dot(grad_up, up_w.T, preferred_element_type=jnp.float32)).astype(jnp.bfloat16)
            return (total + grad_slot.astype(jnp.float32), (grad_gate_w, grad_up_w, grad_down_w))
        grad_normed_two, expert_grads = lax.scan(expert_backward, jnp.zeros((SEQUENCE_LENGTH, MODEL_DIM), jnp.float32), (w_gate, w_up, w_down, coefs))
        gain_mlp_part = lax.optimization_barrier(jnp.sum(grad_normed_two * hat_two, 0))
        grad_hidden = grad_top + norm_backward_step(grad_normed_two, hat_two, inverse_two, gain_mlp)
        grad_att_bf = grad_hidden.astype(jnp.bfloat16)
        grad_w_out = jnp.dot(grad_att_bf.T, attention_half_precision, preferred_element_type=jnp.float32)
        attention_gradient = jnp.dot(grad_att_bf, w_out, preferred_element_type=jnp.float32).astype(jnp.bfloat16)
        gradient_by_group = attention_gradient.reshape(SEQUENCE_LENGTH, KEY_VALUE_HEADS, query_group, HEAD_SIZE).transpose(1, 0, 2, 3)
        attention_by_group = attention_half_precision.reshape(SEQUENCE_LENGTH, KEY_VALUE_HEADS, query_group, HEAD_SIZE).transpose(1, 0, 2, 3)
        logsumexp_by_group = logsumexp_rows.reshape(KEY_VALUE_HEADS, query_group, SEQUENCE_LENGTH)
        grad_q_heads, grad_k_heads, grad_v_heads = lax.map(lambda a: head_backward(a[0], a[1], a[2], positions, a[3], a[4], a[5]), (group_rows, keys_heads, values_heads, logsumexp_by_group, gradient_by_group, attention_by_group))
        grad_queries = grad_q_heads.transpose(1, 0, 2, 3).reshape(SEQUENCE_LENGTH, QUERY_HEADS, HEAD_SIZE)
        grad_keys = grad_k_heads.transpose(1, 0, 2)
        value_gradients = grad_v_heads.transpose(1, 0, 2)
        grad_normed_q = rotate_back(grad_queries, cosine, sine)
        gain_query_part = lax.optimization_barrier(jnp.sum(grad_normed_q * hat_q, (0, 1)))
        grad_q_bf = norm_backward_step(grad_normed_q, hat_q, inverse_q, gain_query).astype(jnp.bfloat16).reshape(SEQUENCE_LENGTH, QUERY_HEADS * HEAD_SIZE)
        normalized_key_gradient = rotate_back(grad_keys, cosine, sine)
        gain_key_part = lax.optimization_barrier(jnp.sum(normalized_key_gradient * key_unit_rows, (0, 1)))
        key_gradient_half = norm_backward_step(normalized_key_gradient, key_unit_rows, key_inverse_radius, key_norm_gain).astype(jnp.bfloat16).reshape(SEQUENCE_LENGTH, KEY_VALUE_HEADS * HEAD_SIZE)
        value_gradient_half = value_gradients.astype(jnp.bfloat16).reshape(SEQUENCE_LENGTH, KEY_VALUE_HEADS * HEAD_SIZE)
        grad_normed_one = jnp.dot(grad_q_bf, w_query.T, preferred_element_type=jnp.float32) + jnp.dot(key_gradient_half, key_matrix.T, preferred_element_type=jnp.float32) + jnp.dot(value_gradient_half, value_matrix.T, preferred_element_type=jnp.float32)
        grad_w_query = jnp.dot(first_normalized.T, grad_q_bf, preferred_element_type=jnp.float32)
        grad_w_key = jnp.dot(first_normalized.T, key_gradient_half, preferred_element_type=jnp.float32)
        grad_w_value = jnp.dot(first_normalized.T, value_gradient_half, preferred_element_type=jnp.float32)
        gain_attn_part = lax.optimization_barrier(jnp.sum(grad_normed_one * hat_one, 0))
        grad_tokens = grad_hidden + norm_backward_step(grad_normed_one, hat_one, inverse_one, gain_attn)
        parts = (gain_attn_part, gain_mlp_part, gain_query_part, gain_key_part, grad_w_query, grad_w_key, grad_w_value, grad_w_out, expert_grads[0], expert_grads[1], expert_grads[2])
        totals = tuple((a + b for a, b in zip(totals, parts)))
        return (totals, (block_out, grad_tokens, logsumexp_rows, route_grad))
    offset_begin = (jnp.zeros((MODEL_DIM,), jnp.float32), jnp.zeros((MODEL_DIM,), jnp.float32), jnp.zeros((HEAD_SIZE,), jnp.float32), jnp.zeros((HEAD_SIZE,), jnp.float32), jnp.zeros((MODEL_DIM, QUERY_HEADS * HEAD_SIZE), jnp.float32), jnp.zeros((MODEL_DIM, KEY_VALUE_HEADS * HEAD_SIZE), jnp.float32), jnp.zeros((MODEL_DIM, KEY_VALUE_HEADS * HEAD_SIZE), jnp.float32), jnp.zeros((MODEL_DIM, QUERY_HEADS * HEAD_SIZE), jnp.float32), jnp.zeros((EXPERT_COUNT, MODEL_DIM, EXPERT_HIDDEN), jnp.float32), jnp.zeros((EXPERT_COUNT, MODEL_DIM, EXPERT_HIDDEN), jnp.float32), jnp.zeros((EXPERT_COUNT, MODEL_DIM, EXPERT_HIDDEN), jnp.float32))
    totals, stacked = lax.scan(one_sequence, offset_begin, (tokens, expert_ids, route_weight, cotangent))
    return (stacked[0], stacked[1], stacked[2], stacked[3], totals[0], totals[1], totals[2], totals[3], totals[4], totals[5], totals[6], totals[7], totals[8], totals[9], totals[10])
```

```python
import functools

import jax
import jax.numpy as jnp
from jax import lax
from jax.experimental import pallas as pl
from jax.experimental.pallas import tpu as pltpu
from jax.sharding import PartitionSpec as P

epsilon = 1e-06
theta_base = 1000000.0
BF = jnp.bfloat16
F32 = jnp.float32


def pairs(count, k):
    return [(i, i ^ k) for i in range(count)]


def swap(value, axis, k):
    return lax.ppermute(value, axis, pairs(lax.axis_size(axis), k))


def order_of(count):
    return sorted(range(1, count), key=lambda k: -bin(k).count("1"))


def collect(value, axis):
    count = lax.axis_size(axis)
    got = {0: value}
    for k in order_of(count):
        got[k] = swap(value, axis, k)
    return [got[k] for k in range(count)]


def folded_positions(rows, count_ctx, half_block):
    block = rows // half_block
    offset = rows % half_block
    device = block // 2
    placed = jnp.where(block % 2 == 0, device, 2 * count_ctx - 1 - device)
    return placed * half_block + offset


def rope_tables(positions, head_dim):
    freq = jnp.arange(head_dim // 2, dtype=F32) * (2.0 / head_dim)
    inverse = jnp.power(jnp.float32(theta_base), -freq)
    angles = positions.astype(F32)[..., None] * inverse
    cosine, sine = jnp.cos(angles), jnp.sin(angles)
    return jnp.concatenate([cosine, cosine], -1), jnp.concatenate([-sine, sine], -1)


def inv_rms(field):
    return lax.rsqrt(jnp.mean(field * field, -1, keepdims=True) + epsilon)


def norm_backward_step(grad_normed, normed_hat, inverse, gain):
    scaled = grad_normed * gain
    return inverse * (scaled - normed_hat * jnp.mean(scaled * normed_hat, -1, keepdims=True))


def mm(a, b):
    return lax.dot_general(a, b, (((1,), (0,)), ((), ())), preferred_element_type=F32)


def mm_nt(a, b):
    return lax.dot_general(a, b, (((1,), (1,)), ((), ())), preferred_element_type=F32)


def mm_tn(a, b):
    return lax.dot_general(a, b, (((0,), (0,)), ((), ())), preferred_element_type=F32)


def turn(u, cosine, sine):
    return u * cosine + pltpu.roll(u, u.shape[-1] // 2, 1) * sine


def turn_back(u, cosine, sine):
    return u * cosine - pltpu.roll(u, u.shape[-1] // 2, 1) * sine


def key_kernel(raw_ref, gain_ref, cos_ref, sin_ref, out_ref):
    dim = gain_ref.shape[-1]
    raw = raw_ref[:, :dim]
    unit = raw * inv_rms(raw)
    out_ref[0] = turn(unit * gain_ref[...], cos_ref[...], sin_ref[...]).astype(BF)
    out_ref[1] = raw_ref[:, dim:].astype(BF)


def key_grad_kernel(count, raw_ref, gain_ref, cos_ref, sin_ref, *refs):
    parts, (out_ref, gain_out) = refs[:count], refs[count:]
    dim = gain_ref.shape[-1]
    total = parts[0][...].astype(F32)
    for part in parts[1:]:
        total = total + part[...].astype(F32)
    raw = raw_ref[:, :dim]
    inverse = inv_rms(raw)
    unit = raw * inverse
    grad = turn_back(total[0], cos_ref[...], sin_ref[...])
    gain_out[...] = jnp.sum(grad * unit, 0, keepdims=True)
    out_ref[:, :dim] = norm_backward_step(grad, unit, inverse, gain_ref[...]).astype(BF)
    out_ref[:, dim:] = total[1].astype(BF)


def natural_rows(me_s, count_s, ref, out_ref):
    own = out_ref.shape[0] // count_s
    for j in range(count_s):
        out_ref[j * own : (j + 1) * own, :] = ref[me_s ^ j, 0]


def gather_keys(me_s, me_c, kv_ref, k_nat, v_nat):
    count_c, _, count_s, _, own, _ = kv_ref.shape
    half = count_s * own // 2
    for jc in range(count_c):
        for j in range(count_s):
            row = j * own
            at = jc * half + row if row < half else (2 * count_c - 1 - jc) * half + row - half
            k_nat[at : at + own, :] = kv_ref[me_c ^ jc, 0, me_s ^ j, 0]
            v_nat[at : at + own, :] = kv_ref[me_c ^ jc, 1, me_s ^ j, 0]


def masks(me_c, count_c, half):
    length = count_c * half
    key = lax.broadcasted_iota(jnp.int32, (length, half), 0)
    lane = lax.broadcasted_iota(jnp.int32, (length, half), 1)
    near = key <= me_c * half + lane
    far = key + length <= (2 * count_c - 1 - me_c) * half + lane
    return near, far


def attn_kernel(ids_ref, q_ref, kv_ref, gain_ref, cos_ref, sin_ref, attn_ref, lse_ref, qb_ref, q_nat, k_nat, v_nat):
    me_s, me_c = ids_ref[0], ids_ref[1]
    count_s, _, own, width = q_ref.shape
    count_c = kv_ref.shape[0]
    dim = gain_ref.shape[-1]
    rows = count_s * own
    half = rows // 2
    length = count_c * half
    scale = dim ** (-0.5)
    natural_rows(me_s, count_s, q_ref, q_nat)
    gather_keys(me_s, me_c, kv_ref, k_nat, v_nat)
    near, far = masks(me_c, count_c, half)
    v_t = v_nat[...].astype(F32).T.astype(BF)
    for h in range(width // dim):
        lanes = slice(h * dim, (h + 1) * dim)
        u = q_nat[:, lanes]
        q = turn(u * inv_rms(u) * gain_ref[...], cos_ref[...], sin_ref[...]).astype(BF)
        qb_ref[0, :, lanes] = q
        s_a = mm_nt(k_nat[:length], q) * scale
        s_n = jnp.where(near, s_a[:, :half], -1e30)
        s_f = s_a[:, half:]
        s_b = jnp.where(far, mm_nt(k_nat[length:], q[half:]) * scale, -1e30)
        m_n = jnp.max(s_n, 0, keepdims=True)
        m_f = jnp.maximum(jnp.max(s_f, 0, keepdims=True), jnp.max(s_b, 0, keepdims=True))
        e_n = jnp.exp(s_n - m_n)
        e_f = jnp.exp(s_f - m_f)
        e_b = jnp.exp(s_b - m_f)
        l_n = jnp.sum(e_n, 0, keepdims=True)
        l_f = jnp.sum(e_f, 0, keepdims=True) + jnp.sum(e_b, 0, keepdims=True)
        lse_ref[0, h : h + 1, :half] = m_n + jnp.log(l_n)
        lse_ref[0, h : h + 1, half:] = m_f + jnp.log(l_f)
        r_n, r_f = 1.0 / l_n, 1.0 / l_f
        o_n = mm(v_t[:, :length], (e_n * r_n).astype(BF))
        o_f = mm(v_t[:, :length], (e_f * r_f).astype(BF)) + mm(v_t[:, length:], (e_b * r_f).astype(BF))
        o = jnp.concatenate([o_n.T, o_f.T], 0).astype(BF)
        for j in range(count_s):
            attn_ref[me_s ^ j, 0, :, lanes] = o[j * own : (j + 1) * own]


def attn_grad_kernel(ids_ref, qb_ref, q_ref, kv_ref, do_ref, attn_ref, lse_ref, gain_ref, cos_ref, sin_ref, gq_ref, dkv_ref, gain_out, q_nat, k_nat, v_nat, do_nat, attn_nat, dk_acc, dv_acc):
    me_s, me_c = ids_ref[0], ids_ref[1]
    count_s, _, own, width = q_ref.shape
    count_c = kv_ref.shape[0]
    dim = gain_ref.shape[-1]
    rows = count_s * own
    half = rows // 2
    length = count_c * half
    scale = dim ** (-0.5)
    natural_rows(me_s, count_s, q_ref, q_nat)
    natural_rows(me_s, count_s, do_ref, do_nat)
    natural_rows(me_s, count_s, attn_ref, attn_nat)
    gather_keys(me_s, me_c, kv_ref, k_nat, v_nat)
    near, far = masks(me_c, count_c, half)
    k_t = k_nat[...].astype(F32).T.astype(BF)
    heads = width // dim
    lane = lax.broadcasted_iota(jnp.int32, (rows, dim), 1)
    delta = jnp.zeros((rows, dim), F32)
    for h in range(heads):
        lanes = slice(h * dim, (h + 1) * dim)
        both = jnp.sum(do_nat[:, lanes].astype(F32) * attn_nat[:, lanes].astype(F32), -1, keepdims=True)
        delta = jnp.where(lane == h, both, delta)
    delta_t = delta.T
    gain_total = jnp.zeros((1, dim), F32)
    for h in range(heads):
        lanes = slice(h * dim, (h + 1) * dim)
        q = qb_ref[0, :, lanes]
        do = do_nat[:, lanes]
        lse = lse_ref[0, h : h + 1, :]
        dlt = delta_t[h : h + 1, :]
        s_a = mm_nt(k_nat[:length], q) * scale
        dp_a = mm_nt(v_nat[:length], do)
        p_n = jnp.exp(jnp.where(near, s_a[:, :half], -1e30) - lse[:, :half])
        p_f = jnp.exp(s_a[:, half:] - lse[:, half:])
        p_a = jnp.concatenate([p_n, p_f], 1)
        ds_a = (p_a * (dp_a - dlt) * scale).astype(BF)
        p_a = p_a.astype(BF)
        s_b = jnp.where(far, mm_nt(k_nat[length:], q[half:]) * scale, -1e30)
        dp_b = mm_nt(v_nat[length:], do[half:])
        p_b = jnp.exp(s_b - lse[:, half:])
        ds_b = (p_b * (dp_b - dlt[:, half:]) * scale).astype(BF)
        p_b = p_b.astype(BF)
        dk_a, dv_a = mm(ds_a, q), mm(p_a, do)
        dk_b, dv_b = mm(ds_b, q[half:]), mm(p_b, do[half:])
        if h == 0:
            dk_acc[:length], dv_acc[:length] = dk_a, dv_a
            dk_acc[length:], dv_acc[length:] = dk_b, dv_b
        else:
            dk_acc[:length] += dk_a
            dv_acc[:length] += dv_a
            dk_acc[length:] += dk_b
            dv_acc[length:] += dv_b
        dq_a = mm(k_t[:, :length], ds_a)
        dq_f = dq_a[:, half:] + mm(k_t[:, length:], ds_b)
        dq = jnp.concatenate([dq_a[:, :half].T, dq_f.T], 0)
        grad = turn_back(dq, cos_ref[...], sin_ref[...])
        u = q_nat[:, lanes]
        inverse = inv_rms(u)
        hat = u * inverse
        gain_total = gain_total + jnp.sum(grad * hat, 0, keepdims=True)
        out = norm_backward_step(grad, hat, inverse, gain_ref[...]).astype(BF)
        for j in range(count_s):
            gq_ref[me_s ^ j, 0, :, lanes] = out[j * own : (j + 1) * own]
    gain_out[0] = gain_total
    for jc in range(count_c):
        for j in range(count_s):
            row = j * own
            at = jc * half + row if row < half else (2 * count_c - 1 - jc) * half + row - half
            dkv_ref[me_c ^ jc, 0, me_s ^ j, 0] = dk_acc[at : at + own, :].astype(BF)
            dkv_ref[me_c ^ jc, 1, me_s ^ j, 0] = dv_acc[at : at + own, :].astype(BF)


def per_device(
    tokens,
    gain_attn,
    gain_mlp,
    gain_query,
    key_norm_gain,
    w_query,
    key_matrix,
    value_matrix,
    w_out,
    w_gate,
    w_up,
    w_down,
    expert_ids,
    route_weight,
    cotangent,
):
    count_c = lax.axis_size("ctx")
    count_s = lax.axis_size("shard")
    me_c = lax.axis_index("ctx")
    me_s = lax.axis_index("shard")
    seqs, block_rows, width = tokens.shape
    own = expert_ids.shape[1]
    head_dim = gain_query.shape[0]
    q_width = w_query.shape[1]
    heads = q_width // head_dim
    hidden_width = w_gate.shape[2]
    half = block_rows // 2
    seq_len = block_rows * count_c
    own_rows = seqs * own
    all_rows = count_s * own_rows
    both = ("ctx", "dp")

    def gather(value):
        return lax.all_gather(value, both, axis=0, tiled=True)

    def scatter(value):
        return lax.psum_scatter(value, both, scatter_dimension=0, tiled=True)

    full_qkv = gather(jnp.concatenate([w_query, key_matrix, value_matrix], 1))
    full_out = gather(w_out)
    full_experts = gather(jnp.concatenate([w_gate[0], w_up[0], w_down[0]], 1))

    rows_at = [
        lax.dynamic_slice_in_dim(tokens, (me_s ^ k) * own, own, 1).reshape(own_rows, width)
        for k in range(count_s)
    ]
    residual = jnp.concatenate(rows_at, 0).astype(F32)
    inverse_one = inv_rms(residual)
    hat_one = residual * inverse_one
    normed_one = (hat_one * gain_attn).astype(BF)
    residual_own = rows_at[0].astype(F32)
    inverse_own = inv_rms(residual_own)
    hat_own = residual_own * inverse_own

    grad_top = cotangent.reshape(own_rows, width)
    grad_all = jnp.concatenate(collect(grad_top, "shard"), 0)
    ids = expert_ids.reshape(own_rows, -1)
    weights = route_weight.reshape(own_rows, -1)

    def weight_for(expert):
        return jnp.sum(jnp.where(ids == expert, weights, 0.0), -1)

    coefs = {0: weight_for(me_s)}
    for k in order_of(count_s):
        coefs[k] = swap(weight_for(me_s ^ k), "shard", k)
    coef = jnp.concatenate([coefs[k] for k in range(count_s)], 0)[:, None]
    grad_rows = (coef * grad_all.astype(F32)).astype(BF)

    block = jnp.arange(count_s, dtype=jnp.int32)
    offsets = jnp.arange(own, dtype=jnp.int32)
    row_natural = me_c * block_rows + jnp.arange(block_rows, dtype=jnp.int32)
    cos_nat, sin_nat = rope_tables(folded_positions(row_natural, count_c, half), head_dim)
    row_peer = me_c * block_rows + (me_s ^ block)[:, None] * own + offsets
    cos_peer, sin_peer = rope_tables(folded_positions(row_peer, count_c, half), head_dim)

    def spread(table):
        return jnp.broadcast_to(
            table[:, None], (count_s, seqs, own, head_dim)
        ).reshape(all_rows, head_dim)

    cos_rows, sin_rows = spread(cos_peer), spread(sin_peer)
    gain_q_row, gain_k_row = gain_query[None], key_norm_gain[None]

    kv_raw = mm(normed_one, full_qkv[:, q_width:])
    kv_own = pl.pallas_call(
        key_kernel, out_shape=jax.ShapeDtypeStruct((2, all_rows, head_dim), BF), name="key_prep"
    )(kv_raw, gain_k_row, cos_rows, sin_rows)
    kv_all = jnp.stack(collect(kv_own, "ctx"), 0).reshape(
        count_c, 2, count_s, seqs, own, head_dim
    )
    queries = mm(normed_one, full_qkv[:, :q_width]).reshape(count_s, seqs, own, q_width)

    me_ids = jnp.stack([me_s, me_c]).astype(jnp.int32)
    row_spec = pl.BlockSpec((count_s, 1, own, q_width), lambda s, _: (0, s, 0, 0))
    kv_spec = pl.BlockSpec(
        (count_c, 2, count_s, 1, own, head_dim), lambda s, _: (0, 0, 0, s, 0, 0)
    )
    nat_spec = pl.BlockSpec((1, block_rows, q_width), lambda s, _: (s, 0, 0))
    lse_spec = pl.BlockSpec((1, heads, block_rows), lambda s, _: (s, 0, 0))

    def whole(shape):
        return pl.BlockSpec(shape, lambda s, _: (0,) * len(shape))

    table_spec = whole((block_rows, head_dim))
    gain_spec = whole((1, head_dim))
    attn, lse, queries_bf = pl.pallas_call(
        attn_kernel,
        grid_spec=pltpu.PrefetchScalarGridSpec(
            num_scalar_prefetch=1,
            grid=(seqs,),
            in_specs=[row_spec, kv_spec, gain_spec, table_spec, table_spec],
            out_specs=[row_spec, lse_spec, nat_spec],
            scratch_shapes=[
                pltpu.VMEM((block_rows, q_width), F32),
                pltpu.VMEM((seq_len, head_dim), BF),
                pltpu.VMEM((seq_len, head_dim), BF),
            ],
        ),
        out_shape=[
            jax.ShapeDtypeStruct((count_s, seqs, own, q_width), BF),
            jax.ShapeDtypeStruct((seqs, heads, block_rows), F32),
            jax.ShapeDtypeStruct((seqs, block_rows, q_width), BF),
        ],
        name="attn_fwd",
        cost_estimate=pl.CostEstimate(
            flops=4 * all_rows * seq_len * q_width, bytes_accessed=16 * all_rows * q_width, transcendentals=0
        ),
    )(me_ids, queries, kv_all, gain_q_row, cos_nat, sin_nat)

    def reduce_blocks(block_of):
        got = {k: swap(block_of(k).astype(BF), "shard", k) for k in order_of(count_s)}
        total = block_of(0)
        for k in range(1, count_s):
            total = total + got[k].astype(F32)
        return total

    attended = reduce_blocks(lambda k: mm_nt(attn[k].reshape(own_rows, q_width), full_out))
    hidden = residual_own + attended
    inverse_two = inv_rms(hidden)
    hat_two = hidden * inverse_two
    normed_two = (hat_two * gain_mlp).astype(BF)
    arrived = jnp.concatenate(collect(normed_two, "shard"), 0)

    full_gate_up = full_experts[:, : 2 * hidden_width]
    full_down = full_experts[:, 2 * hidden_width :]
    grad_inner = mm(grad_rows, full_down)
    pre = mm(arrived, full_gate_up)
    gate_pre, up_pre = pre[:, :hidden_width], pre[:, hidden_width:]
    gate_sig = jax.nn.sigmoid(gate_pre)
    gate_act = gate_pre * gate_sig
    inner_bf = (gate_act * up_pre).astype(BF)
    grad_gate = grad_inner * up_pre * gate_sig * (1.0 + gate_pre * (1.0 - gate_sig))
    grad_up = grad_inner * gate_act
    grad_gate_up = jnp.concatenate([grad_gate.astype(BF), grad_up.astype(BF)], 1)
    grad_slots = mm_nt(grad_gate_up, full_gate_up)
    grad_normed_two = reduce_blocks(lambda k: grad_slots[k * own_rows : (k + 1) * own_rows])
    grad_w_experts = jnp.concatenate(
        [mm_tn(arrived, grad_gate_up).astype(BF), mm_tn(grad_rows, inner_bf).astype(BF)], 1
    )
    sum_experts = scatter(grad_w_experts).astype(F32)

    expert_out = mm_nt(inner_bf, full_down).astype(BF).astype(F32)
    weighted = coef * expert_out
    mixture = reduce_blocks(lambda k: weighted[k * own_rows : (k + 1) * own_rows])
    block_out = (hidden + mixture).astype(BF)
    route_part = jnp.sum(grad_all.astype(F32) * expert_out, -1)
    route_all = {0: route_part[:own_rows]}
    for k in order_of(count_s):
        route_all[k] = swap(route_part[k * own_rows : (k + 1) * own_rows], "shard", k)
    route_grad = jnp.zeros(ids.shape, F32)
    for k in range(count_s):
        route_grad = jnp.where(ids == (me_s ^ k), route_all[k][:, None], route_grad)

    gain_mlp_part = jnp.sum(grad_normed_two * hat_two, 0)
    grad_hidden = grad_top.astype(F32) + norm_backward_step(
        grad_normed_two, hat_two, inverse_two, gain_mlp
    )
    grad_att = jnp.concatenate(collect(grad_hidden.astype(BF), "shard"), 0)
    attention_gradient = mm(grad_att, full_out).astype(BF)
    sum_out = scatter(mm_tn(grad_att, attn.reshape(all_rows, q_width)).astype(BF)).astype(F32)

    grad_q, grad_kv, gain_q_parts = pl.pallas_call(
        attn_grad_kernel,
        grid_spec=pltpu.PrefetchScalarGridSpec(
            num_scalar_prefetch=1,
            grid=(seqs,),
            in_specs=[
                nat_spec, row_spec, kv_spec, row_spec, row_spec, lse_spec,
                gain_spec, table_spec, table_spec,
            ],
            out_specs=[row_spec, kv_spec, pl.BlockSpec((1, 1, head_dim), lambda s, _: (s, 0, 0))],
            scratch_shapes=[
                pltpu.VMEM((block_rows, q_width), F32),
                pltpu.VMEM((seq_len, head_dim), BF),
                pltpu.VMEM((seq_len, head_dim), BF),
                pltpu.VMEM((block_rows, q_width), BF),
                pltpu.VMEM((block_rows, q_width), BF),
                pltpu.VMEM((seq_len, head_dim), F32),
                pltpu.VMEM((seq_len, head_dim), F32),
            ],
        ),
        out_shape=[
            jax.ShapeDtypeStruct((count_s, seqs, own, q_width), BF),
            jax.ShapeDtypeStruct((count_c, 2, count_s, seqs, own, head_dim), BF),
            jax.ShapeDtypeStruct((seqs, 1, head_dim), F32),
        ],
        name="attn_bwd",
        cost_estimate=pl.CostEstimate(
            flops=10 * all_rows * seq_len * q_width, bytes_accessed=32 * all_rows * q_width, transcendentals=0
        ),
    )(
        me_ids, queries_bf, queries, kv_all,
        attention_gradient.reshape(count_s, seqs, own, q_width),
        attn, lse, gain_q_row, cos_nat, sin_nat,
    )
    grad_kv = grad_kv.reshape(count_c, 2, all_rows, head_dim)
    kv_parts = [grad_kv[0]] + [swap(grad_kv[k], "ctx", k) for k in range(1, count_c)]
    grad_kv_bf, gain_k_part = pl.pallas_call(
        functools.partial(key_grad_kernel, count_c),
        out_shape=[
            jax.ShapeDtypeStruct((all_rows, 2 * head_dim), BF),
            jax.ShapeDtypeStruct((1, head_dim), F32),
        ],
        name="key_grad",
    )(kv_raw, gain_k_row, cos_rows, sin_rows, *kv_parts)

    grad_q = grad_q.reshape(all_rows, q_width)
    grad_qkv = jnp.concatenate([grad_q, grad_kv_bf], 1)
    sum_qkv = scatter(mm_tn(normed_one, grad_qkv).astype(BF)).astype(F32)
    grad_normed_one = reduce_blocks(
        lambda k: mm_nt(grad_qkv[k * own_rows : (k + 1) * own_rows], full_qkv)
    )
    gain_attn_part = jnp.sum(grad_normed_one * hat_own, 0)
    grad_tokens = grad_hidden + norm_backward_step(
        grad_normed_one, hat_own, inverse_own, gain_attn
    )
    gains = jnp.concatenate(
        [gain_attn_part, gain_mlp_part, jnp.sum(gain_q_parts, (0, 1)), gain_k_part[0]]
    ).reshape(-1, head_dim)
    for axis in ("dp", "shard", "ctx"):
        step = 1
        while step < lax.axis_size(axis):
            gains = gains + swap(gains, axis, step)
            step *= 2
    gains = gains.reshape(-1)

    def own_shape(value):
        return value.reshape(seqs, own, value.shape[-1])

    return (
        own_shape(block_out),
        own_shape(grad_tokens),
        lse,
        own_shape(route_grad),
        gains[:width],
        gains[width : 2 * width],
        gains[2 * width : 2 * width + head_dim],
        gains[2 * width + head_dim :],
        sum_qkv[:, :q_width],
        sum_qkv[:, q_width : q_width + head_dim],
        sum_qkv[:, q_width + head_dim :],
        sum_out,
        sum_experts[None, :, :hidden_width],
        sum_experts[None, :, hidden_width : 2 * hidden_width],
        sum_experts[None, :, 2 * hidden_width :],
    )


def solution(mesh):
    placed = (
        P("dp", "ctx", None),
        P(),
        P(),
        P(),
        P(),
        P(("ctx", "dp"), "shard"),
        P(("ctx", "dp"), "shard"),
        P(("ctx", "dp"), "shard"),
        P(("ctx", "dp"), "shard"),
        P("shard", ("ctx", "dp"), None),
        P("shard", ("ctx", "dp"), None),
        P("shard", ("ctx", "dp"), None),
        P("dp", ("ctx", "shard"), None),
        P("dp", ("ctx", "shard"), None),
        P("dp", ("ctx", "shard"), None),
    )
    return jax.shard_map(
        per_device,
        mesh=mesh,
        in_specs=placed,
        out_specs=(
            P("dp", ("ctx", "shard"), None),
            P("dp", ("ctx", "shard"), None),
            P("dp", "shard", "ctx"),
            P("dp", ("ctx", "shard"), None),
            P(),
            P(),
            P(),
            P(),
            P(("ctx", "dp"), "shard"),
            P(("ctx", "dp"), "shard"),
            P(("ctx", "dp"), "shard"),
            P(("ctx", "dp"), "shard"),
            P("shard", ("ctx", "dp"), None),
            P("shard", ("ctx", "dp"), None),
            P("shard", ("ctx", "dp"), None),
        ),
        check_vma=False,
    )
```

```python
import functools

import jax
import jax.numpy as jnp
from jax import lax
from jax.experimental import pallas as pl
from jax.experimental.pallas import tpu as pltpu
from jax.sharding import PartitionSpec as P

epsilon = 1e-06
theta_base = 1000000.0
BF = jnp.bfloat16
F32 = jnp.float32


def pairs(count, k):
    return [(i, i ^ k) for i in range(count)]


def swap(value, axis, k):
    return lax.ppermute(value, axis, pairs(lax.axis_size(axis), k))


def order_of(count):
    return sorted(range(1, count), key=lambda k: -bin(k).count("1"))


def collect(value, axis):
    count = lax.axis_size(axis)
    got = {0: value}
    for k in order_of(count):
        got[k] = swap(value, axis, k)
    return [got[k] for k in range(count)]


def folded_positions(rows, count_ctx, half_block):
    block = rows // half_block
    offset = rows % half_block
    device = block // 2
    placed = jnp.where(block % 2 == 0, device, 2 * count_ctx - 1 - device)
    return placed * half_block + offset


def rope_tables(positions, head_dim):
    freq = jnp.arange(head_dim // 2, dtype=F32) * (2.0 / head_dim)
    inverse = jnp.power(jnp.float32(theta_base), -freq)
    angles = positions.astype(F32)[..., None] * inverse
    cosine, sine = jnp.cos(angles), jnp.sin(angles)
    return jnp.concatenate([cosine, cosine], -1), jnp.concatenate([-sine, sine], -1)


def inv_rms(field):
    return lax.rsqrt(jnp.mean(field * field, -1, keepdims=True) + epsilon)


def norm_backward_step(grad_normed, normed_hat, inverse, gain):
    scaled = grad_normed * gain
    return inverse * (scaled - normed_hat * jnp.mean(scaled * normed_hat, -1, keepdims=True))


def mm(a, b):
    return lax.dot_general(a, b, (((1,), (0,)), ((), ())), preferred_element_type=F32)


def mm_nt(a, b):
    return lax.dot_general(a, b, (((1,), (1,)), ((), ())), preferred_element_type=F32)


def mm_tn(a, b):
    return lax.dot_general(a, b, (((0,), (0,)), ((), ())), preferred_element_type=F32)


def turn(u, cosine, sine):
    return u * cosine + pltpu.roll(u, u.shape[-1] // 2, 1) * sine


def turn_back(u, cosine, sine):
    return u * cosine - pltpu.roll(u, u.shape[-1] // 2, 1) * sine


def key_kernel(raw_ref, gain_ref, cos_ref, sin_ref, out_ref):
    dim = gain_ref.shape[-1]
    raw = raw_ref[:, :dim]
    unit = raw * inv_rms(raw)
    out_ref[0] = turn(unit * gain_ref[...], cos_ref[...], sin_ref[...]).astype(BF)
    out_ref[1] = raw_ref[:, dim:].astype(BF)


def key_grad_kernel(count, raw_ref, gain_ref, cos_ref, sin_ref, *refs):
    parts, (out_ref, gain_out) = refs[:count], refs[count:]
    dim = gain_ref.shape[-1]
    total = parts[0][...].astype(F32)
    for part in parts[1:]:
        total = total + part[...].astype(F32)
    raw = raw_ref[:, :dim]
    inverse = inv_rms(raw)
    unit = raw * inverse
    grad = turn_back(total[0], cos_ref[...], sin_ref[...])
    gain_out[...] = jnp.sum(grad * unit, 0, keepdims=True)
    out_ref[:, :dim] = norm_backward_step(grad, unit, inverse, gain_ref[...]).astype(BF)
    out_ref[:, dim:] = total[1].astype(BF)


def natural_rows(me_s, count_s, ref, out_ref):
    own = out_ref.shape[0] // count_s
    for j in range(count_s):
        out_ref[j * own : (j + 1) * own, :] = ref[me_s ^ j, 0]


def gather_keys(me_s, me_c, kv_ref, k_nat, v_nat):
    count_c, _, count_s, _, own, _ = kv_ref.shape
    half = count_s * own // 2
    for jc in range(count_c):
        for j in range(count_s):
            row = j * own
            at = jc * half + row if row < half else (2 * count_c - 1 - jc) * half + row - half
            k_nat[at : at + own, :] = kv_ref[me_c ^ jc, 0, me_s ^ j, 0]
            v_nat[at : at + own, :] = kv_ref[me_c ^ jc, 1, me_s ^ j, 0]


def masks(me_c, count_c, half):
    length = count_c * half
    key = lax.broadcasted_iota(jnp.int32, (length, half), 0)
    lane = lax.broadcasted_iota(jnp.int32, (length, half), 1)
    near = key <= me_c * half + lane
    far = key + length <= (2 * count_c - 1 - me_c) * half + lane
    return near, far


def attn_kernel(ids_ref, q_ref, kv_ref, gain_ref, cos_ref, sin_ref, attn_ref, lse_ref, qb_ref, q_nat, k_nat, v_nat):
    me_s, me_c = ids_ref[0], ids_ref[1]
    count_s, _, own, width = q_ref.shape
    count_c = kv_ref.shape[0]
    dim = gain_ref.shape[-1]
    rows = count_s * own
    half = rows // 2
    length = count_c * half
    scale = dim ** (-0.5)
    natural_rows(me_s, count_s, q_ref, q_nat)
    gather_keys(me_s, me_c, kv_ref, k_nat, v_nat)
    near, far = masks(me_c, count_c, half)
    v_t = v_nat[...].astype(F32).T.astype(BF)
    for h in range(width // dim):
        lanes = slice(h * dim, (h + 1) * dim)
        u = q_nat[:, lanes]
        q = turn(u * inv_rms(u) * gain_ref[...], cos_ref[...], sin_ref[...]).astype(BF)
        qb_ref[0, :, lanes] = q
        s_a = mm_nt(k_nat[:length], q) * scale
        s_n = jnp.where(near, s_a[:, :half], -1e30)
        s_f = s_a[:, half:]
        s_b = jnp.where(far, mm_nt(k_nat[length:], q[half:]) * scale, -1e30)
        m_n = jnp.max(s_n, 0, keepdims=True)
        m_f = jnp.maximum(jnp.max(s_f, 0, keepdims=True), jnp.max(s_b, 0, keepdims=True))
        e_n = jnp.exp(s_n - m_n)
        e_f = jnp.exp(s_f - m_f)
        e_b = jnp.exp(s_b - m_f)
        l_n = jnp.sum(e_n, 0, keepdims=True)
        l_f = jnp.sum(e_f, 0, keepdims=True) + jnp.sum(e_b, 0, keepdims=True)
        lse_ref[0, h : h + 1, :half] = m_n + jnp.log(l_n)
        lse_ref[0, h : h + 1, half:] = m_f + jnp.log(l_f)
        r_n, r_f = 1.0 / l_n, 1.0 / l_f
        o_n = mm(v_t[:, :length], (e_n * r_n).astype(BF))
        o_f = mm(v_t[:, :length], (e_f * r_f).astype(BF)) + mm(v_t[:, length:], (e_b * r_f).astype(BF))
        o = jnp.concatenate([o_n.T, o_f.T], 0).astype(BF)
        for j in range(count_s):
            attn_ref[me_s ^ j, 0, :, lanes] = o[j * own : (j + 1) * own]


def attn_grad_kernel(ids_ref, qb_ref, q_ref, kv_ref, do_ref, attn_ref, lse_ref, gain_ref, cos_ref, sin_ref, gq_ref, dkv_ref, gain_out, q_nat, k_nat, v_nat, do_nat, attn_nat, dk_acc, dv_acc):
    me_s, me_c = ids_ref[0], ids_ref[1]
    count_s, _, own, width = q_ref.shape
    count_c = kv_ref.shape[0]
    dim = gain_ref.shape[-1]
    rows = count_s * own
    half = rows // 2
    length = count_c * half
    scale = dim ** (-0.5)
    natural_rows(me_s, count_s, q_ref, q_nat)
    natural_rows(me_s, count_s, do_ref, do_nat)
    natural_rows(me_s, count_s, attn_ref, attn_nat)
    gather_keys(me_s, me_c, kv_ref, k_nat, v_nat)
    near, far = masks(me_c, count_c, half)
    k_t = k_nat[...].astype(F32).T.astype(BF)
    heads = width // dim
    lane = lax.broadcasted_iota(jnp.int32, (rows, dim), 1)
    delta = jnp.zeros((rows, dim), F32)
    for h in range(heads):
        lanes = slice(h * dim, (h + 1) * dim)
        both = jnp.sum(do_nat[:, lanes].astype(F32) * attn_nat[:, lanes].astype(F32), -1, keepdims=True)
        delta = jnp.where(lane == h, both, delta)
    delta_t = delta.T
    gain_total = jnp.zeros((1, dim), F32)
    for h in range(heads):
        lanes = slice(h * dim, (h + 1) * dim)
        q = qb_ref[0, :, lanes]
        do = do_nat[:, lanes]
        lse = lse_ref[0, h : h + 1, :]
        dlt = delta_t[h : h + 1, :]
        s_a = mm_nt(k_nat[:length], q) * scale
        dp_a = mm_nt(v_nat[:length], do)
        p_n = jnp.exp(jnp.where(near, s_a[:, :half], -1e30) - lse[:, :half])
        p_f = jnp.exp(s_a[:, half:] - lse[:, half:])
        p_a = jnp.concatenate([p_n, p_f], 1)
        ds_a = (p_a * (dp_a - dlt) * scale).astype(BF)
        p_a = p_a.astype(BF)
        s_b = jnp.where(far, mm_nt(k_nat[length:], q[half:]) * scale, -1e30)
        dp_b = mm_nt(v_nat[length:], do[half:])
        p_b = jnp.exp(s_b - lse[:, half:])
        ds_b = (p_b * (dp_b - dlt[:, half:]) * scale).astype(BF)
        p_b = p_b.astype(BF)
        dk_a, dv_a = mm(ds_a, q), mm(p_a, do)
        dk_b, dv_b = mm(ds_b, q[half:]), mm(p_b, do[half:])
        if h == 0:
            dk_acc[:length], dv_acc[:length] = dk_a, dv_a
            dk_acc[length:], dv_acc[length:] = dk_b, dv_b
        else:
            dk_acc[:length] += dk_a
            dv_acc[:length] += dv_a
            dk_acc[length:] += dk_b
            dv_acc[length:] += dv_b
        dq_a = mm(k_t[:, :length], ds_a)
        dq_f = dq_a[:, half:] + mm(k_t[:, length:], ds_b)
        dq = jnp.concatenate([dq_a[:, :half].T, dq_f.T], 0)
        grad = turn_back(dq, cos_ref[...], sin_ref[...])
        u = q_nat[:, lanes]
        inverse = inv_rms(u)
        hat = u * inverse
        gain_total = gain_total + jnp.sum(grad * hat, 0, keepdims=True)
        out = norm_backward_step(grad, hat, inverse, gain_ref[...]).astype(BF)
        for j in range(count_s):
            gq_ref[me_s ^ j, 0, :, lanes] = out[j * own : (j + 1) * own]
    gain_out[0] = gain_total
    for jc in range(count_c):
        for j in range(count_s):
            row = j * own
            at = jc * half + row if row < half else (2 * count_c - 1 - jc) * half + row - half
            dkv_ref[me_c ^ jc, 0, me_s ^ j, 0] = dk_acc[at : at + own, :].astype(BF)
            dkv_ref[me_c ^ jc, 1, me_s ^ j, 0] = dv_acc[at : at + own, :].astype(BF)


def expert_grad_kernel(rows_ref, grad_in_ref, grads_ref, inner_ref, out_ref):
    wide = grads_ref.shape[1]
    out_ref[:, :wide] = mm_tn(rows_ref[...], grads_ref[...]).astype(BF)
    out_ref[:, wide:] = mm_tn(grad_in_ref[...], inner_ref[...]).astype(BF)


def expert_grads(rows, grad_in, grads, inner):
    count, width = rows.shape
    tile = 256 if width % 256 == 0 else width
    wide = grads.shape[1] + inner.shape[1]

    def resident(value):
        return pl.BlockSpec(value.shape, lambda i: (0, 0))

    return pl.pallas_call(
        expert_grad_kernel,
        grid=(width // tile,),
        in_specs=[
            pl.BlockSpec((count, tile), lambda i: (0, i)),
            pl.BlockSpec((count, tile), lambda i: (0, i)),
            resident(grads),
            resident(inner),
        ],
        out_specs=pl.BlockSpec((tile, wide), lambda i: (i, 0)),
        out_shape=jax.ShapeDtypeStruct((width, wide), BF),
        name="expert_grads",
        cost_estimate=pl.CostEstimate(
            flops=2 * count * width * wide, bytes_accessed=4 * (count + wide) * width, transcendentals=0
        ),
    )(rows, grad_in, grads, inner)


def after(value, *others):
    return lax.optimization_barrier((value, *others))[0]


def per_device(
    tokens,
    gain_attn,
    gain_mlp,
    gain_query,
    key_norm_gain,
    w_query,
    key_matrix,
    value_matrix,
    w_out,
    w_gate,
    w_up,
    w_down,
    expert_ids,
    route_weight,
    cotangent,
):
    count_c = lax.axis_size("ctx")
    count_s = lax.axis_size("shard")
    me_c = lax.axis_index("ctx")
    me_s = lax.axis_index("shard")
    seqs, block_rows, width = tokens.shape
    own = expert_ids.shape[1]
    head_dim = gain_query.shape[0]
    q_width = w_query.shape[1]
    heads = q_width // head_dim
    hidden_width = w_gate.shape[2]
    half = block_rows // 2
    seq_len = block_rows * count_c
    own_rows = seqs * own
    all_rows = count_s * own_rows
    both = ("ctx", "dp")

    def gather(value):
        return lax.all_gather(value, both, axis=0, tiled=True)

    def scatter(value):
        return lax.psum_scatter(value, both, scatter_dimension=0, tiled=True)

    full_qkv = gather(jnp.concatenate([w_query, key_matrix, value_matrix], 1))
    full_out = gather(w_out)
    full_experts = gather(jnp.concatenate([w_gate[0], w_up[0], w_down[0]], 1))

    rows_at = [
        lax.dynamic_slice_in_dim(tokens, (me_s ^ k) * own, own, 1).reshape(own_rows, width)
        for k in range(count_s)
    ]
    residual = jnp.concatenate(rows_at, 0).astype(F32)
    inverse_one = inv_rms(residual)
    hat_one = residual * inverse_one
    normed_one = (hat_one * gain_attn).astype(BF)
    residual_own = rows_at[0].astype(F32)
    inverse_own = inv_rms(residual_own)
    hat_own = residual_own * inverse_own

    grad_top = cotangent.reshape(own_rows, width)
    grad_all = jnp.concatenate(collect(grad_top, "shard"), 0)
    ids = expert_ids.reshape(own_rows, -1)
    weights = route_weight.reshape(own_rows, -1)

    def weight_for(expert):
        return jnp.sum(jnp.where(ids == expert, weights, 0.0), -1)

    coefs = {0: weight_for(me_s)}
    for k in order_of(count_s):
        coefs[k] = swap(weight_for(me_s ^ k), "shard", k)
    coef = jnp.concatenate([coefs[k] for k in range(count_s)], 0)[:, None]
    grad_rows = (coef * grad_all.astype(F32)).astype(BF)

    block = jnp.arange(count_s, dtype=jnp.int32)
    offsets = jnp.arange(own, dtype=jnp.int32)
    row_natural = me_c * block_rows + jnp.arange(block_rows, dtype=jnp.int32)
    cos_nat, sin_nat = rope_tables(folded_positions(row_natural, count_c, half), head_dim)
    row_peer = me_c * block_rows + (me_s ^ block)[:, None] * own + offsets
    cos_peer, sin_peer = rope_tables(folded_positions(row_peer, count_c, half), head_dim)

    def spread(table):
        return jnp.broadcast_to(
            table[:, None], (count_s, seqs, own, head_dim)
        ).reshape(all_rows, head_dim)

    cos_rows, sin_rows = spread(cos_peer), spread(sin_peer)
    gain_q_row, gain_k_row = gain_query[None], key_norm_gain[None]

    normed_one = after(normed_one, grad_rows)
    kv_raw = mm(normed_one, full_qkv[:, q_width:])
    kv_own = pl.pallas_call(
        key_kernel, out_shape=jax.ShapeDtypeStruct((2, all_rows, head_dim), BF), name="key_prep"
    )(kv_raw, gain_k_row, cos_rows, sin_rows)
    kv_all = jnp.stack(collect(kv_own, "ctx"), 0).reshape(
        count_c, 2, count_s, seqs, own, head_dim
    )
    queries = mm(normed_one, full_qkv[:, :q_width]).reshape(count_s, seqs, own, q_width)

    me_ids = jnp.stack([me_s, me_c]).astype(jnp.int32)
    row_spec = pl.BlockSpec((count_s, 1, own, q_width), lambda s, _: (0, s, 0, 0))
    kv_spec = pl.BlockSpec(
        (count_c, 2, count_s, 1, own, head_dim), lambda s, _: (0, 0, 0, s, 0, 0)
    )
    nat_spec = pl.BlockSpec((1, block_rows, q_width), lambda s, _: (s, 0, 0))
    lse_spec = pl.BlockSpec((1, heads, block_rows), lambda s, _: (s, 0, 0))

    def whole(shape):
        return pl.BlockSpec(shape, lambda s, _: (0,) * len(shape))

    table_spec = whole((block_rows, head_dim))
    gain_spec = whole((1, head_dim))
    attn, lse, queries_bf = pl.pallas_call(
        attn_kernel,
        grid_spec=pltpu.PrefetchScalarGridSpec(
            num_scalar_prefetch=1,
            grid=(seqs,),
            in_specs=[row_spec, kv_spec, gain_spec, table_spec, table_spec],
            out_specs=[row_spec, lse_spec, nat_spec],
            scratch_shapes=[
                pltpu.VMEM((block_rows, q_width), F32),
                pltpu.VMEM((seq_len, head_dim), BF),
                pltpu.VMEM((seq_len, head_dim), BF),
            ],
        ),
        out_shape=[
            jax.ShapeDtypeStruct((count_s, seqs, own, q_width), BF),
            jax.ShapeDtypeStruct((seqs, heads, block_rows), F32),
            jax.ShapeDtypeStruct((seqs, block_rows, q_width), BF),
        ],
        name="attn_fwd",
        cost_estimate=pl.CostEstimate(
            flops=4 * all_rows * seq_len * q_width, bytes_accessed=16 * all_rows * q_width, transcendentals=0
        ),
    )(me_ids, queries, kv_all, gain_q_row, cos_nat, sin_nat)

    def reduce_blocks(block_of):
        got = {k: swap(block_of(k).astype(BF), "shard", k) for k in order_of(count_s)}
        total = block_of(0).astype(F32)
        for k in range(1, count_s):
            total = total + got[k].astype(F32)
        return total

    attended = reduce_blocks(lambda k: mm_nt(attn[k].reshape(own_rows, q_width), full_out))
    hidden = residual_own + attended
    inverse_two = inv_rms(hidden)
    hat_two = hidden * inverse_two
    normed_two = (hat_two * gain_mlp).astype(BF)
    arrived = jnp.concatenate(collect(normed_two, "shard"), 0)

    full_gate_up = full_experts[:, : 2 * hidden_width]
    full_down = full_experts[:, 2 * hidden_width :]
    grad_inner = mm(grad_rows, full_down)
    pre = mm(arrived, full_gate_up)
    gate_pre, up_pre = pre[:, :hidden_width], pre[:, hidden_width:]
    gate_sig = jax.nn.sigmoid(gate_pre)
    gate_act = gate_pre * gate_sig
    inner_bf = (gate_act * up_pre).astype(BF)
    grad_gate = grad_inner * up_pre * gate_sig * (1.0 + gate_pre * (1.0 - gate_sig))
    grad_up = grad_inner * gate_act
    grad_gate_up = jnp.concatenate([grad_gate.astype(BF), grad_up.astype(BF)], 1)
    grad_slots = mm_nt(grad_gate_up, full_gate_up)
    grad_normed_two = reduce_blocks(lambda k: grad_slots[k * own_rows : (k + 1) * own_rows])
    grad_w_experts = expert_grads(arrived, grad_rows, grad_gate_up, inner_bf)
    sum_experts = scatter(grad_w_experts).astype(F32)

    gain_mlp_part = jnp.sum(grad_normed_two * hat_two, 0)
    grad_hidden = grad_top.astype(F32) + norm_backward_step(
        grad_normed_two, hat_two, inverse_two, gain_mlp
    )
    expert_out = mm_nt(inner_bf, full_down).astype(BF).astype(F32)
    weighted = coef * expert_out
    weighted = weighted.astype(BF)
    route_part = jnp.sum(grad_all.astype(F32) * expert_out, -1)
    grad_hidden_bf = after(grad_hidden.astype(BF), grad_w_experts)
    grad_att = jnp.concatenate(collect(grad_hidden_bf, "shard"), 0)
    grad_att, weighted, route_part = lax.optimization_barrier((grad_att, weighted, route_part))
    mixture = reduce_blocks(lambda k: weighted[k * own_rows : (k + 1) * own_rows])
    block_out = (hidden + mixture).astype(BF)
    route_all = {0: route_part[:own_rows]}
    for k in order_of(count_s):
        route_all[k] = swap(route_part[k * own_rows : (k + 1) * own_rows], "shard", k)
    route_grad = jnp.zeros(ids.shape, F32)
    for k in range(count_s):
        route_grad = jnp.where(ids == (me_s ^ k), route_all[k][:, None], route_grad)

    attention_gradient = mm(grad_att, full_out).astype(BF)

    grad_q, grad_kv, gain_q_parts = pl.pallas_call(
        attn_grad_kernel,
        grid_spec=pltpu.PrefetchScalarGridSpec(
            num_scalar_prefetch=1,
            grid=(seqs,),
            in_specs=[
                nat_spec, row_spec, kv_spec, row_spec, row_spec, lse_spec,
                gain_spec, table_spec, table_spec,
            ],
            out_specs=[row_spec, kv_spec, pl.BlockSpec((1, 1, head_dim), lambda s, _: (s, 0, 0))],
            scratch_shapes=[
                pltpu.VMEM((block_rows, q_width), F32),
                pltpu.VMEM((seq_len, head_dim), BF),
                pltpu.VMEM((seq_len, head_dim), BF),
                pltpu.VMEM((block_rows, q_width), BF),
                pltpu.VMEM((block_rows, q_width), BF),
                pltpu.VMEM((seq_len, head_dim), F32),
                pltpu.VMEM((seq_len, head_dim), F32),
            ],
        ),
        out_shape=[
            jax.ShapeDtypeStruct((count_s, seqs, own, q_width), BF),
            jax.ShapeDtypeStruct((count_c, 2, count_s, seqs, own, head_dim), BF),
            jax.ShapeDtypeStruct((seqs, 1, head_dim), F32),
        ],
        name="attn_bwd",
        cost_estimate=pl.CostEstimate(
            flops=10 * all_rows * seq_len * q_width, bytes_accessed=32 * all_rows * q_width, transcendentals=0
        ),
    )(
        me_ids, queries_bf, queries, kv_all,
        attention_gradient.reshape(count_s, seqs, own, q_width),
        attn, lse, gain_q_row, cos_nat, sin_nat,
    )
    grad_w_out = mm_tn(after(grad_att, grad_kv), attn.reshape(all_rows, q_width)).astype(BF)
    sum_out = scatter(grad_w_out).astype(F32)
    grad_kv = grad_kv.reshape(count_c, 2, all_rows, head_dim)
    kv_parts = [grad_kv[0]] + [swap(grad_kv[k], "ctx", k) for k in range(1, count_c)]
    grad_kv_bf, gain_k_part = pl.pallas_call(
        functools.partial(key_grad_kernel, count_c),
        out_shape=[
            jax.ShapeDtypeStruct((all_rows, 2 * head_dim), BF),
            jax.ShapeDtypeStruct((1, head_dim), F32),
        ],
        name="key_grad",
    )(kv_raw, gain_k_row, cos_rows, sin_rows, *kv_parts)

    grad_q = grad_q.reshape(all_rows, q_width)
    grad_qkv = jnp.concatenate([grad_q, grad_kv_bf], 1)
    sum_qkv = scatter(mm_tn(normed_one, grad_qkv).astype(BF)).astype(F32)
    grad_normed_one = reduce_blocks(
        lambda k: mm_nt(grad_qkv[k * own_rows : (k + 1) * own_rows], full_qkv)
    )
    gain_attn_part = jnp.sum(grad_normed_one * hat_own, 0)
    grad_tokens = grad_hidden + norm_backward_step(
        grad_normed_one, hat_own, inverse_own, gain_attn
    )
    gains = jnp.concatenate(
        [gain_attn_part, gain_mlp_part, jnp.sum(gain_q_parts, (0, 1)), gain_k_part[0]]
    ).reshape(-1, head_dim)
    for axis in ("dp", "shard", "ctx"):
        step = 1
        while step < lax.axis_size(axis):
            gains = gains + swap(gains, axis, step)
            step *= 2
    gains = gains.reshape(-1)

    def own_shape(value):
        return value.reshape(seqs, own, value.shape[-1])

    return (
        own_shape(block_out),
        own_shape(grad_tokens),
        lse,
        own_shape(route_grad),
        gains[:width],
        gains[width : 2 * width],
        gains[2 * width : 2 * width + head_dim],
        gains[2 * width + head_dim :],
        sum_qkv[:, :q_width],
        sum_qkv[:, q_width : q_width + head_dim],
        sum_qkv[:, q_width + head_dim :],
        sum_out,
        sum_experts[None, :, :hidden_width],
        sum_experts[None, :, hidden_width : 2 * hidden_width],
        sum_experts[None, :, 2 * hidden_width :],
    )


def solution(mesh):
    placed = (
        P("dp", "ctx", None),
        P(),
        P(),
        P(),
        P(),
        P(("ctx", "dp"), "shard"),
        P(("ctx", "dp"), "shard"),
        P(("ctx", "dp"), "shard"),
        P(("ctx", "dp"), "shard"),
        P("shard", ("ctx", "dp"), None),
        P("shard", ("ctx", "dp"), None),
        P("shard", ("ctx", "dp"), None),
        P("dp", ("ctx", "shard"), None),
        P("dp", ("ctx", "shard"), None),
        P("dp", ("ctx", "shard"), None),
    )
    return jax.shard_map(
        per_device,
        mesh=mesh,
        in_specs=placed,
        out_specs=(
            P("dp", ("ctx", "shard"), None),
            P("dp", ("ctx", "shard"), None),
            P("dp", "shard", "ctx"),
            P("dp", ("ctx", "shard"), None),
            P(),
            P(),
            P(),
            P(),
            P(("ctx", "dp"), "shard"),
            P(("ctx", "dp"), "shard"),
            P(("ctx", "dp"), "shard"),
            P(("ctx", "dp"), "shard"),
            P("shard", ("ctx", "dp"), None),
            P("shard", ("ctx", "dp"), None),
            P("shard", ("ctx", "dp"), None),
        ),
        check_vma=False,
    )
```

```python
import functools

import jax
import jax.numpy as jnp
from jax import lax
from jax.experimental import pallas as pl
from jax.experimental.pallas import tpu as pltpu
from jax.sharding import PartitionSpec as P


epsilon = 1e-06
theta_base = 1000000.0
BF = jnp.bfloat16
F32 = jnp.float32


def pairs(count, k):
    return [(i, i ^ k) for i in range(count)]


def swap(value, axis, k):
    return lax.ppermute(value, axis, pairs(lax.axis_size(axis), k))


def order_of(count):
    return sorted(range(1, count), key=lambda k: -bin(k).count("1"))


def collect(value, axis):
    count = lax.axis_size(axis)
    got = {0: value}
    for k in order_of(count):
        got[k] = swap(value, axis, k)
    return [got[k] for k in range(count)]


def folded_positions(rows, count_ctx, half_block):
    block = rows // half_block
    offset = rows % half_block
    device = block // 2
    placed = jnp.where(block % 2 == 0, device, 2 * count_ctx - 1 - device)
    return placed * half_block + offset


def rope_tables(positions, head_dim):
    freq = jnp.arange(head_dim // 2, dtype=F32) * (2.0 / head_dim)
    inverse = jnp.power(jnp.float32(theta_base), -freq)
    angles = positions.astype(F32)[..., None] * inverse
    cosine, sine = jnp.cos(angles), jnp.sin(angles)
    return jnp.concatenate([cosine, cosine], -1), jnp.concatenate([-sine, sine], -1)


def inv_rms(field):
    return lax.rsqrt(jnp.mean(field * field, -1, keepdims=True) + epsilon)


def norm_backward_step(grad_normed, normed_hat, inverse, gain):
    scaled = grad_normed * gain
    return inverse * (scaled - normed_hat * jnp.mean(scaled * normed_hat, -1, keepdims=True))


def mm(a, b):
    return lax.dot_general(a, b, (((1,), (0,)), ((), ())), preferred_element_type=F32)


def mm_nt(a, b):
    return lax.dot_general(a, b, (((1,), (1,)), ((), ())), preferred_element_type=F32)


def mm_tn(a, b):
    return lax.dot_general(a, b, (((0,), (0,)), ((), ())), preferred_element_type=F32)


def turn(u, cosine, sine):
    return u * cosine + pltpu.roll(u, u.shape[-1] // 2, 1) * sine


def turn_back(u, cosine, sine):
    return u * cosine - pltpu.roll(u, u.shape[-1] // 2, 1) * sine


def key_kernel(raw_ref, gain_ref, cos_ref, sin_ref, out_ref):
    dim = gain_ref.shape[-1]
    raw = raw_ref[:, :dim]
    unit = raw * inv_rms(raw)
    out_ref[0] = turn(unit * gain_ref[...], cos_ref[...], sin_ref[...]).astype(BF)
    out_ref[1] = raw_ref[:, dim:].astype(BF)


def key_grad_kernel(count, raw_ref, gain_ref, cos_ref, sin_ref, *refs):
    parts, (out_ref, gain_out) = refs[:count], refs[count:]
    dim = gain_ref.shape[-1]
    total = parts[0][...].astype(F32)
    for part in parts[1:]:
        total = total + part[...].astype(F32)
    raw = raw_ref[:, :dim]
    inverse = inv_rms(raw)
    unit = raw * inverse
    grad = turn_back(total[0], cos_ref[...], sin_ref[...])
    gain_out[...] = jnp.sum(grad * unit, 0, keepdims=True)
    out_ref[:, :dim] = norm_backward_step(grad, unit, inverse, gain_ref[...]).astype(BF)
    out_ref[:, dim:] = total[1].astype(BF)


def natural_rows(me_s, count_s, ref, out_ref):
    own = out_ref.shape[0] // count_s
    for j in range(count_s):
        out_ref[j * own : (j + 1) * own, :] = ref[me_s ^ j, 0]


def gather_keys(me_s, me_c, kv_ref, k_nat, v_nat):
    count_c, _, count_s, _, own, _ = kv_ref.shape
    half = count_s * own // 2
    for jc in range(count_c):
        for j in range(count_s):
            row = j * own
            at = jc * half + row if row < half else (2 * count_c - 1 - jc) * half + row - half
            k_nat[at : at + own, :] = kv_ref[me_c ^ jc, 0, me_s ^ j, 0]
            v_nat[at : at + own, :] = kv_ref[me_c ^ jc, 1, me_s ^ j, 0]


def masks(me_c, count_c, half):
    length = count_c * half
    key = lax.broadcasted_iota(jnp.int32, (length, half), 0)
    lane = lax.broadcasted_iota(jnp.int32, (length, half), 1)
    near = key <= me_c * half + lane
    far = key + length <= (2 * count_c - 1 - me_c) * half + lane
    return near, far


def attn_kernel(ids_ref, q_ref, kv_ref, gain_ref, cos_ref, sin_ref, attn_ref, lse_ref, qb_ref, q_nat, k_nat, v_nat):
    me_s, me_c = ids_ref[0], ids_ref[1]
    count_s, _, own, width = q_ref.shape
    count_c = kv_ref.shape[0]
    dim = gain_ref.shape[-1]
    rows = count_s * own
    half = rows // 2
    length = count_c * half
    scale = dim ** (-0.5)
    natural_rows(me_s, count_s, q_ref, q_nat)
    gather_keys(me_s, me_c, kv_ref, k_nat, v_nat)
    near, far = masks(me_c, count_c, half)
    v_t = v_nat[...].astype(F32).T.astype(BF)
    for h in range(width // dim):
        lanes = slice(h * dim, (h + 1) * dim)
        u = q_nat[:, lanes]
        q = turn(u * inv_rms(u) * gain_ref[...], cos_ref[...], sin_ref[...]).astype(BF)
        qb_ref[0, :, lanes] = q
        s_a = mm_nt(k_nat[:length], q) * scale
        s_n = jnp.where(near, s_a[:, :half], -1e30)
        s_f = s_a[:, half:]
        s_b = jnp.where(far, mm_nt(k_nat[length:], q[half:]) * scale, -1e30)
        m_n = jnp.max(s_n, 0, keepdims=True)
        m_f = jnp.maximum(jnp.max(s_f, 0, keepdims=True), jnp.max(s_b, 0, keepdims=True))
        e_n = jnp.exp(s_n - m_n)
        e_f = jnp.exp(s_f - m_f)
        e_b = jnp.exp(s_b - m_f)
        l_n = jnp.sum(e_n, 0, keepdims=True)
        l_f = jnp.sum(e_f, 0, keepdims=True) + jnp.sum(e_b, 0, keepdims=True)
        lse_ref[0, h : h + 1, :half] = m_n + jnp.log(l_n)
        lse_ref[0, h : h + 1, half:] = m_f + jnp.log(l_f)
        r_n, r_f = 1.0 / l_n, 1.0 / l_f
        o_n = mm(v_t[:, :length], (e_n * r_n).astype(BF))
        o_f = mm(v_t[:, :length], (e_f * r_f).astype(BF)) + mm(v_t[:, length:], (e_b * r_f).astype(BF))
        o = jnp.concatenate([o_n.T, o_f.T], 0).astype(BF)
        for j in range(count_s):
            attn_ref[me_s ^ j, 0, :, lanes] = o[j * own : (j + 1) * own]


def attn_grad_kernel(ids_ref, qb_ref, q_ref, kv_ref, do_ref, attn_ref, lse_ref, gain_ref, cos_ref, sin_ref, gq_ref, dkv_ref, gain_out, q_nat, k_nat, v_nat, do_nat, attn_nat, dk_acc, dv_acc):
    me_s, me_c = ids_ref[0], ids_ref[1]
    count_s, _, own, width = q_ref.shape
    count_c = kv_ref.shape[0]
    dim = gain_ref.shape[-1]
    rows = count_s * own
    half = rows // 2
    length = count_c * half
    scale = dim ** (-0.5)
    natural_rows(me_s, count_s, q_ref, q_nat)
    natural_rows(me_s, count_s, do_ref, do_nat)
    natural_rows(me_s, count_s, attn_ref, attn_nat)
    gather_keys(me_s, me_c, kv_ref, k_nat, v_nat)
    near, far = masks(me_c, count_c, half)
    k_t = k_nat[...].astype(F32).T.astype(BF)
    heads = width // dim
    lane = lax.broadcasted_iota(jnp.int32, (rows, dim), 1)
    delta = jnp.zeros((rows, dim), F32)
    for h in range(heads):
        lanes = slice(h * dim, (h + 1) * dim)
        both = jnp.sum(do_nat[:, lanes].astype(F32) * attn_nat[:, lanes].astype(F32), -1, keepdims=True)
        delta = jnp.where(lane == h, both, delta)
    delta_t = delta.T
    gain_total = jnp.zeros((1, dim), F32)
    for h in range(heads):
        lanes = slice(h * dim, (h + 1) * dim)
        q = qb_ref[0, :, lanes]
        do = do_nat[:, lanes]
        lse = lse_ref[0, h : h + 1, :]
        dlt = delta_t[h : h + 1, :]
        s_a = mm_nt(k_nat[:length], q) * scale
        dp_a = mm_nt(v_nat[:length], do)
        p_n = jnp.exp(jnp.where(near, s_a[:, :half], -1e30) - lse[:, :half])
        p_f = jnp.exp(s_a[:, half:] - lse[:, half:])
        p_a = jnp.concatenate([p_n, p_f], 1)
        ds_a = (p_a * (dp_a - dlt) * scale).astype(BF)
        p_a = p_a.astype(BF)
        s_b = jnp.where(far, mm_nt(k_nat[length:], q[half:]) * scale, -1e30)
        dp_b = mm_nt(v_nat[length:], do[half:])
        p_b = jnp.exp(s_b - lse[:, half:])
        ds_b = (p_b * (dp_b - dlt[:, half:]) * scale).astype(BF)
        p_b = p_b.astype(BF)
        dk_a, dv_a = mm(ds_a, q), mm(p_a, do)
        dk_b, dv_b = mm(ds_b, q[half:]), mm(p_b, do[half:])
        if h == 0:
            dk_acc[:length], dv_acc[:length] = dk_a, dv_a
            dk_acc[length:], dv_acc[length:] = dk_b, dv_b
        else:
            dk_acc[:length] += dk_a
            dv_acc[:length] += dv_a
            dk_acc[length:] += dk_b
            dv_acc[length:] += dv_b
        dq_a = mm(k_t[:, :length], ds_a)
        dq_f = dq_a[:, half:] + mm(k_t[:, length:], ds_b)
        dq = jnp.concatenate([dq_a[:, :half].T, dq_f.T], 0)
        grad = turn_back(dq, cos_ref[...], sin_ref[...])
        u = q_nat[:, lanes]
        inverse = inv_rms(u)
        hat = u * inverse
        gain_total = gain_total + jnp.sum(grad * hat, 0, keepdims=True)
        out = norm_backward_step(grad, hat, inverse, gain_ref[...]).astype(BF)
        for j in range(count_s):
            gq_ref[me_s ^ j, 0, :, lanes] = out[j * own : (j + 1) * own]
    gain_out[0] = gain_total
    for jc in range(count_c):
        for j in range(count_s):
            row = j * own
            at = jc * half + row if row < half else (2 * count_c - 1 - jc) * half + row - half
            dkv_ref[me_c ^ jc, 0, me_s ^ j, 0] = dk_acc[at : at + own, :].astype(BF)
            dkv_ref[me_c ^ jc, 1, me_s ^ j, 0] = dv_acc[at : at + own, :].astype(BF)


def expert_grad_kernel(rows_ref, grad_in_ref, grads_ref, inner_ref, out_ref):
    wide = grads_ref.shape[1]
    out_ref[:, :wide] = mm_tn(rows_ref[...], grads_ref[...]).astype(BF)
    out_ref[:, wide:] = mm_tn(grad_in_ref[...], inner_ref[...]).astype(BF)


def expert_grads(rows, grad_in, grads, inner):
    count, width = rows.shape
    tile = 256 if width % 256 == 0 else width
    wide = grads.shape[1] + inner.shape[1]

    def resident(value):
        return pl.BlockSpec(value.shape, lambda i: (0, 0))

    return pl.pallas_call(
        expert_grad_kernel,
        grid=(width // tile,),
        in_specs=[
            pl.BlockSpec((count, tile), lambda i: (0, i)),
            pl.BlockSpec((count, tile), lambda i: (0, i)),
            resident(grads),
            resident(inner),
        ],
        out_specs=pl.BlockSpec((tile, wide), lambda i: (i, 0)),
        out_shape=jax.ShapeDtypeStruct((width, wide), BF),
        name="expert_grads",
        cost_estimate=pl.CostEstimate(
            flops=2 * count * width * wide, bytes_accessed=4 * (count + wide) * width, transcendentals=0
        ),
    )(rows, grad_in, grads, inner)


def after(value, *others):
    return lax.optimization_barrier((value, *others))[0]


def per_device(
    tokens,
    gain_attn,
    gain_mlp,
    gain_query,
    key_norm_gain,
    w_query,
    key_matrix,
    value_matrix,
    w_out,
    w_gate,
    w_up,
    w_down,
    expert_ids,
    route_weight,
    cotangent,
):
    count_c = lax.axis_size("ctx")
    count_s = lax.axis_size("shard")
    me_c = lax.axis_index("ctx")
    me_s = lax.axis_index("shard")
    seqs, block_rows, width = tokens.shape
    own = expert_ids.shape[1]
    head_dim = gain_query.shape[0]
    q_width = w_query.shape[1]
    heads = q_width // head_dim
    hidden_width = w_gate.shape[2]
    half = block_rows // 2
    seq_len = block_rows * count_c
    own_rows = seqs * own
    all_rows = count_s * own_rows
    both = ("ctx", "dp")

    def gather(value):
        return lax.all_gather(value, both, axis=0, tiled=True)

    def scatter(value):
        return lax.psum_scatter(value, both, scatter_dimension=0, tiled=True)

    def sum_cores(value):
        count_d = lax.axis_size("dp")
        me_d = lax.axis_index("dp")
        parts = value.reshape(count_c, count_d, -1, value.shape[1])
        total = lax.dynamic_index_in_dim(parts, me_d, 1, False).astype(F32)
        for k in range(1, count_d):
            sent = lax.dynamic_index_in_dim(parts, me_d ^ k, 1, False)
            total = total + swap(sent, "dp", k).astype(F32)
        return total.astype(BF)

    def sum_ctx(total):
        result = lax.dynamic_index_in_dim(total, me_c, 0, False).astype(F32)
        for k in order_of(count_c):
            sent = lax.dynamic_index_in_dim(total, me_c ^ k, 0, False)
            result = result + swap(sent, "ctx", k).astype(F32)
        return result

    full_qkv = gather(jnp.concatenate([w_query, key_matrix, value_matrix], 1))
    full_out = gather(w_out)
    full_experts = gather(jnp.concatenate([w_gate[0], w_up[0], w_down[0]], 1))

    rows_at = [
        lax.dynamic_slice_in_dim(tokens, (me_s ^ k) * own, own, 1).reshape(own_rows, width)
        for k in range(count_s)
    ]
    residual = jnp.concatenate(rows_at, 0).astype(F32)
    inverse_one = inv_rms(residual)
    hat_one = residual * inverse_one
    normed_one = (hat_one * gain_attn).astype(BF)
    residual_own = rows_at[0].astype(F32)
    inverse_own = inv_rms(residual_own)
    hat_own = residual_own * inverse_own

    grad_top = cotangent.reshape(own_rows, width)
    grad_all = jnp.concatenate(collect(grad_top, "shard"), 0)
    ids = expert_ids.reshape(own_rows, -1)
    weights = route_weight.reshape(own_rows, -1)

    def weight_for(expert):
        return jnp.sum(jnp.where(ids == expert, weights, 0.0), -1)

    coefs = {0: weight_for(me_s)}
    for k in order_of(count_s):
        coefs[k] = swap(weight_for(me_s ^ k), "shard", k)
    coef = jnp.concatenate([coefs[k] for k in range(count_s)], 0)[:, None]
    grad_rows = (coef * grad_all.astype(F32)).astype(BF)

    block = jnp.arange(count_s, dtype=jnp.int32)
    offsets = jnp.arange(own, dtype=jnp.int32)
    row_natural = me_c * block_rows + jnp.arange(block_rows, dtype=jnp.int32)
    cos_nat, sin_nat = rope_tables(folded_positions(row_natural, count_c, half), head_dim)
    row_peer = me_c * block_rows + (me_s ^ block)[:, None] * own + offsets
    cos_peer, sin_peer = rope_tables(folded_positions(row_peer, count_c, half), head_dim)

    def spread(table):
        return jnp.broadcast_to(
            table[:, None], (count_s, seqs, own, head_dim)
        ).reshape(all_rows, head_dim)

    cos_rows, sin_rows = spread(cos_peer), spread(sin_peer)
    gain_q_row, gain_k_row = gain_query[None], key_norm_gain[None]

    normed_one = after(normed_one, grad_rows)
    kv_raw = mm(normed_one, full_qkv[:, q_width:])
    kv_own = pl.pallas_call(
        key_kernel, out_shape=jax.ShapeDtypeStruct((2, all_rows, head_dim), BF), name="key_prep"
    )(kv_raw, gain_k_row, cos_rows, sin_rows)
    kv_all = jnp.stack(collect(kv_own, "ctx"), 0).reshape(
        count_c, 2, count_s, seqs, own, head_dim
    )
    full_query = full_qkv[:, :q_width]
    queries = mm(normed_one, full_query).reshape(count_s, seqs, own, q_width)
    kv_weights = jnp.concatenate(collect(full_qkv[:, q_width:], "shard"), 1)

    me_ids = jnp.stack([me_s, me_c]).astype(jnp.int32)
    row_spec = pl.BlockSpec((count_s, 1, own, q_width), lambda s, _: (0, s, 0, 0))
    kv_spec = pl.BlockSpec(
        (count_c, 2, count_s, 1, own, head_dim), lambda s, _: (0, 0, 0, s, 0, 0)
    )
    nat_spec = pl.BlockSpec((1, block_rows, q_width), lambda s, _: (s, 0, 0))
    lse_spec = pl.BlockSpec((1, heads, block_rows), lambda s, _: (s, 0, 0))

    def whole(shape):
        return pl.BlockSpec(shape, lambda s, _: (0,) * len(shape))

    table_spec = whole((block_rows, head_dim))
    gain_spec = whole((1, head_dim))
    me_ids, kv_weights = lax.optimization_barrier((me_ids, kv_weights))
    attn, lse, queries_bf = pl.pallas_call(
        attn_kernel,
        grid_spec=pltpu.PrefetchScalarGridSpec(
            num_scalar_prefetch=1,
            grid=(seqs,),
            in_specs=[row_spec, kv_spec, gain_spec, table_spec, table_spec],
            out_specs=[row_spec, lse_spec, nat_spec],
            scratch_shapes=[
                pltpu.VMEM((block_rows, q_width), F32),
                pltpu.VMEM((seq_len, head_dim), BF),
                pltpu.VMEM((seq_len, head_dim), BF),
            ],
        ),
        out_shape=[
            jax.ShapeDtypeStruct((count_s, seqs, own, q_width), BF),
            jax.ShapeDtypeStruct((seqs, heads, block_rows), F32),
            jax.ShapeDtypeStruct((seqs, block_rows, q_width), BF),
        ],
        name="attn_fwd",
        cost_estimate=pl.CostEstimate(
            flops=4 * all_rows * seq_len * q_width, bytes_accessed=16 * all_rows * q_width, transcendentals=0
        ),
    )(me_ids, queries, kv_all, gain_q_row, cos_nat, sin_nat)

    def reduce_blocks(block_of):
        got = {}
        for k in order_of(count_s):
            got[k] = swap(block_of(k).astype(BF), "shard", k)
        total = block_of(0).astype(F32)
        for k in range(1, count_s):
            total = total + got[k].astype(F32)
        return total

    attended = reduce_blocks(lambda k: mm_nt(attn[k].reshape(own_rows, q_width), full_out))
    hidden = residual_own + attended
    inverse_two = inv_rms(hidden)
    hat_two = hidden * inverse_two
    normed_two = (hat_two * gain_mlp).astype(BF)
    arrived = jnp.concatenate(collect(normed_two, "shard"), 0)

    full_gate_up = full_experts[:, : 2 * hidden_width]
    full_down = full_experts[:, 2 * hidden_width :]
    grad_inner = mm(grad_rows, full_down)
    pre = mm(arrived, full_gate_up)
    gate_pre, up_pre = pre[:, :hidden_width], pre[:, hidden_width:]
    gate_sig = jax.nn.sigmoid(gate_pre)
    gate_act = gate_pre * gate_sig
    inner_bf = (gate_act * up_pre).astype(BF)
    grad_gate = grad_inner * up_pre * gate_sig * (1.0 + gate_pre * (1.0 - gate_sig))
    grad_up = grad_inner * gate_act
    grad_gate_up = jnp.concatenate([grad_gate.astype(BF), grad_up.astype(BF)], 1)
    grad_slots = mm_nt(grad_gate_up, full_gate_up)
    grad_normed_two = reduce_blocks(lambda k: grad_slots[k * own_rows : (k + 1) * own_rows])
    grad_w_experts = expert_grads(arrived, grad_rows, after(grad_gate_up, grad_slots), inner_bf)
    sum_experts = scatter(grad_w_experts).astype(F32)

    gain_mlp_part = jnp.sum(grad_normed_two * hat_two, 0)
    grad_hidden = grad_top.astype(F32) + norm_backward_step(
        grad_normed_two, hat_two, inverse_two, gain_mlp
    )
    expert_out = mm_nt(inner_bf, full_down).astype(BF).astype(F32)
    weighted = coef * expert_out
    weighted = weighted.astype(BF)
    route_part = jnp.sum(grad_all.astype(F32) * expert_out, -1)
    grad_hidden_bf = after(grad_hidden.astype(BF), grad_w_experts)
    grad_att = jnp.concatenate(collect(grad_hidden_bf, "shard"), 0)
    grad_att, weighted, route_part = lax.optimization_barrier((grad_att, weighted, route_part))
    mixture = reduce_blocks(lambda k: weighted[k * own_rows : (k + 1) * own_rows])
    block_out = (hidden + mixture).astype(BF)
    route_all = {0: route_part[:own_rows]}
    for k in order_of(count_s):
        route_all[k] = swap(route_part[k * own_rows : (k + 1) * own_rows], "shard", k)
    route_grad = jnp.zeros(ids.shape, F32)
    for k in range(count_s):
        route_grad = jnp.where(ids == (me_s ^ k), route_all[k][:, None], route_grad)

    attention_gradient = mm(grad_att, full_out).astype(BF)

    grad_q, grad_kv, gain_q_parts = pl.pallas_call(
        attn_grad_kernel,
        grid_spec=pltpu.PrefetchScalarGridSpec(
            num_scalar_prefetch=1,
            grid=(seqs,),
            in_specs=[
                nat_spec, row_spec, kv_spec, row_spec, row_spec, lse_spec,
                gain_spec, table_spec, table_spec,
            ],
            out_specs=[row_spec, kv_spec, pl.BlockSpec((1, 1, head_dim), lambda s, _: (s, 0, 0))],
            scratch_shapes=[
                pltpu.VMEM((block_rows, q_width), F32),
                pltpu.VMEM((seq_len, head_dim), BF),
                pltpu.VMEM((seq_len, head_dim), BF),
                pltpu.VMEM((block_rows, q_width), BF),
                pltpu.VMEM((block_rows, q_width), BF),
                pltpu.VMEM((seq_len, head_dim), F32),
                pltpu.VMEM((seq_len, head_dim), F32),
            ],
        ),
        out_shape=[
            jax.ShapeDtypeStruct((count_s, seqs, own, q_width), BF),
            jax.ShapeDtypeStruct((count_c, 2, count_s, seqs, own, head_dim), BF),
            jax.ShapeDtypeStruct((seqs, 1, head_dim), F32),
        ],
        name="attn_bwd",
        cost_estimate=pl.CostEstimate(
            flops=10 * all_rows * seq_len * q_width, bytes_accessed=32 * all_rows * q_width, transcendentals=0
        ),
    )(
        me_ids, queries_bf, queries, kv_all,
        attention_gradient.reshape(count_s, seqs, own, q_width),
        attn, lse, gain_q_row, cos_nat, sin_nat,
    )
    grad_kv = grad_kv.reshape(count_c, 2, all_rows, head_dim)
    grad_q = grad_q.reshape(all_rows, q_width)
    grad_w_query = mm_tn(normed_one, grad_q).astype(BF)
    sum_query = scatter(grad_w_query).astype(F32)
    query_part = reduce_blocks(
        lambda k: mm_nt(grad_q[k * own_rows : (k + 1) * own_rows], full_query)
    )
    grad_w_out = mm_tn(after(grad_att, grad_kv), attn.reshape(all_rows, q_width)).astype(BF)
    half_sum_out = sum_cores(grad_w_out)
    sum_out = sum_ctx(half_sum_out)

    kv_parts = [grad_kv[0]]
    for k in range(1, count_c):
        kv_parts.append(swap(grad_kv[k], "ctx", k))
    kv_parts = list(lax.optimization_barrier((*kv_parts, half_sum_out))[:count_c])
    grad_kv_bf, gain_k_part = pl.pallas_call(
        functools.partial(key_grad_kernel, count_c),
        out_shape=[
            jax.ShapeDtypeStruct((all_rows, 2 * head_dim), BF),
            jax.ShapeDtypeStruct((1, head_dim), F32),
        ],
        name="key_grad",
    )(kv_raw, gain_k_row, cos_rows, sin_rows, *kv_parts)
    kv_rows = {
        k: swap(grad_kv_bf[k * own_rows : (k + 1) * own_rows], "shard", k)
        for k in order_of(count_s)
    }
    kv_rows[0] = grad_kv_bf[:own_rows]
    sum_kv = sum_ctx(sum_cores(mm_tn(normed_one, grad_kv_bf).astype(BF)))
    grad_normed_one = query_part + mm_nt(
        jnp.concatenate([kv_rows[k] for k in range(count_s)], 1), kv_weights
    )
    gain_attn_part = jnp.sum(grad_normed_one * hat_own, 0)
    grad_tokens = grad_hidden + norm_backward_step(
        grad_normed_one, hat_own, inverse_own, gain_attn
    )
    gains = jnp.concatenate(
        [gain_attn_part, gain_mlp_part, jnp.sum(gain_q_parts, (0, 1)), gain_k_part[0]]
    ).reshape(-1, head_dim)
    for axis in ("dp", "shard", "ctx"):
        step = 1
        while step < lax.axis_size(axis):
            gains = gains + swap(gains, axis, step)
            step *= 2
    gains = gains.reshape(-1)

    def own_shape(value):
        return value.reshape(seqs, own, value.shape[-1])

    return (
        own_shape(block_out),
        own_shape(grad_tokens),
        lse,
        own_shape(route_grad),
        gains[:width],
        gains[width : 2 * width],
        gains[2 * width : 2 * width + head_dim],
        gains[2 * width + head_dim :],
        sum_query,
        sum_kv[:, :head_dim],
        sum_kv[:, head_dim:],
        sum_out,
        sum_experts[None, :, :hidden_width],
        sum_experts[None, :, hidden_width : 2 * hidden_width],
        sum_experts[None, :, 2 * hidden_width :],
    )


def solution(mesh):
    placed = (
        P("dp", "ctx", None),
        P(),
        P(),
        P(),
        P(),
        P(("ctx", "dp"), "shard"),
        P(("ctx", "dp"), "shard"),
        P(("ctx", "dp"), "shard"),
        P(("ctx", "dp"), "shard"),
        P("shard", ("ctx", "dp"), None),
        P("shard", ("ctx", "dp"), None),
        P("shard", ("ctx", "dp"), None),
        P("dp", ("ctx", "shard"), None),
        P("dp", ("ctx", "shard"), None),
        P("dp", ("ctx", "shard"), None),
    )

    return jax.shard_map(
        per_device,
        mesh=mesh,
        in_specs=placed,
        out_specs=(
            P("dp", ("ctx", "shard"), None),
            P("dp", ("ctx", "shard"), None),
            P("dp", "shard", "ctx"),
            P("dp", ("ctx", "shard"), None),
            P(),
            P(),
            P(),
            P(),
            P(("ctx", "dp"), "shard"),
            P(("ctx", "dp"), "shard"),
            P(("ctx", "dp"), "shard"),
            P(("ctx", "dp"), "shard"),
            P("shard", ("ctx", "dp"), None),
            P("shard", ("ctx", "dp"), None),
            P("shard", ("ctx", "dp"), None),
        ),
        check_vma=False,
    )
```

```python
import functools

import jax
import jax.numpy as jnp
from jax import lax
from jax.experimental import pallas as pl
from jax.experimental.pallas import tpu as pltpu
from jax.sharding import PartitionSpec as P


epsilon = 1e-06
theta_base = 1000000.0
BF = jnp.bfloat16
F32 = jnp.float32


def pairs(count, k):
    return [(i, i ^ k) for i in range(count)]


def swap(value, axis, k):
    return lax.ppermute(value, axis, pairs(lax.axis_size(axis), k))


def order_of(count):
    return sorted(range(1, count), key=lambda k: -bin(k).count("1"))


def collect(value, axis):
    count = lax.axis_size(axis)
    got = {0: value}
    for k in order_of(count):
        got[k] = swap(value, axis, k)
    return [got[k] for k in range(count)]


def collect_crossed(value, axis):
    if lax.axis_size(axis) != 4:
        return jnp.concatenate(collect(value, axis), 0)
    half = value.shape[1] // 2
    low, high = value[:, :half], value[:, half:]

    def send(part, k):
        return swap(part, axis, k)

    low_1, high_2 = send(low, 1), send(high, 2)
    high_1, low_2 = send(high, 1), send(low, 2)
    low_3, high_3 = swap(low_1, axis, 2), swap(high_2, axis, 1)
    lows = jnp.concatenate([low, low_1, low_2, low_3], 0)
    highs = jnp.concatenate([high, high_1, high_2, high_3], 0)
    return jnp.concatenate([lows, highs], 1)


def folded_positions(rows, count_ctx, half_block):
    block = rows // half_block
    offset = rows % half_block
    device = block // 2
    placed = jnp.where(block % 2 == 0, device, 2 * count_ctx - 1 - device)
    return placed * half_block + offset


def rope_tables(positions, head_dim):
    freq = jnp.arange(head_dim // 2, dtype=F32) * (2.0 / head_dim)
    inverse = jnp.power(jnp.float32(theta_base), -freq)
    angles = positions.astype(F32)[..., None] * inverse
    cosine, sine = jnp.cos(angles), jnp.sin(angles)
    return jnp.concatenate([cosine, cosine], -1), jnp.concatenate([-sine, sine], -1)


def inv_rms(field):
    return lax.rsqrt(jnp.mean(field * field, -1, keepdims=True) + epsilon)


def norm_backward_step(grad_normed, normed_hat, inverse, gain):
    scaled = grad_normed * gain
    return inverse * (scaled - normed_hat * jnp.mean(scaled * normed_hat, -1, keepdims=True))


def mm(a, b):
    return lax.dot_general(a, b, (((1,), (0,)), ((), ())), preferred_element_type=F32)


def mm_nt(a, b):
    return lax.dot_general(a, b, (((1,), (1,)), ((), ())), preferred_element_type=F32)


def mm_tn(a, b):
    return lax.dot_general(a, b, (((0,), (0,)), ((), ())), preferred_element_type=F32)


def turn(u, cosine, sine):
    return u * cosine + pltpu.roll(u, u.shape[-1] // 2, 1) * sine


def turn_back(u, cosine, sine):
    return u * cosine - pltpu.roll(u, u.shape[-1] // 2, 1) * sine


def key_kernel(raw_ref, gain_ref, cos_ref, sin_ref, out_ref):
    dim = gain_ref.shape[-1]
    raw = raw_ref[:, :dim]
    unit = raw * inv_rms(raw)
    out_ref[0] = turn(unit * gain_ref[...], cos_ref[...], sin_ref[...]).astype(BF)
    out_ref[1] = raw_ref[:, dim:].astype(BF)


def key_grad_kernel(count, raw_ref, gain_ref, cos_ref, sin_ref, *refs):
    parts, (out_ref, gain_out) = refs[:count], refs[count:]
    dim = gain_ref.shape[-1]
    total = parts[0][...].astype(F32)
    for part in parts[1:]:
        total = total + part[...].astype(F32)
    raw = raw_ref[:, :dim]
    inverse = inv_rms(raw)
    unit = raw * inverse
    grad = turn_back(total[0], cos_ref[...], sin_ref[...])
    gain_out[...] = jnp.sum(grad * unit, 0, keepdims=True)
    out_ref[:, :dim] = norm_backward_step(grad, unit, inverse, gain_ref[...]).astype(BF)
    out_ref[:, dim:] = total[1].astype(BF)


def natural_rows(me_s, count_s, ref, out_ref):
    own = out_ref.shape[0] // count_s
    for j in range(count_s):
        out_ref[j * own : (j + 1) * own, :] = ref[me_s ^ j, 0]


def gather_keys(me_s, me_c, kv_ref, k_nat, v_nat):
    count_c, _, count_s, _, own, _ = kv_ref.shape
    half = count_s * own // 2
    for jc in range(count_c):
        for j in range(count_s):
            row = j * own
            at = jc * half + row if row < half else (2 * count_c - 1 - jc) * half + row - half
            k_nat[at : at + own, :] = kv_ref[me_c ^ jc, 0, me_s ^ j, 0]
            v_nat[at : at + own, :] = kv_ref[me_c ^ jc, 1, me_s ^ j, 0]


def masks(me_c, count_c, half):
    length = count_c * half
    key = lax.broadcasted_iota(jnp.int32, (length, half), 0)
    lane = lax.broadcasted_iota(jnp.int32, (length, half), 1)
    near = key <= me_c * half + lane
    far = key + length <= (2 * count_c - 1 - me_c) * half + lane
    return near, far


def attn_kernel(ids_ref, q_ref, kv_ref, gain_ref, cos_ref, sin_ref, attn_ref, lse_ref, qb_ref, q_nat, k_nat, v_nat):
    me_s, me_c = ids_ref[0], ids_ref[1]
    count_s, _, own, width = q_ref.shape
    count_c = kv_ref.shape[0]
    dim = gain_ref.shape[-1]
    rows = count_s * own
    half = rows // 2
    length = count_c * half
    scale = dim ** (-0.5)
    natural_rows(me_s, count_s, q_ref, q_nat)
    gather_keys(me_s, me_c, kv_ref, k_nat, v_nat)
    near, far = masks(me_c, count_c, half)
    v_t = v_nat[...].astype(F32).T.astype(BF)
    for h in range(width // dim):
        lanes = slice(h * dim, (h + 1) * dim)
        u = q_nat[:, lanes]
        q = turn(u * inv_rms(u) * gain_ref[...], cos_ref[...], sin_ref[...]).astype(BF)
        qb_ref[0, :, lanes] = q
        s_a = mm_nt(k_nat[:length], q) * scale
        s_n = jnp.where(near, s_a[:, :half], -1e30)
        s_f = s_a[:, half:]
        s_b = jnp.where(far, mm_nt(k_nat[length:], q[half:]) * scale, -1e30)
        m_n = jnp.max(s_n, 0, keepdims=True)
        m_f = jnp.maximum(jnp.max(s_f, 0, keepdims=True), jnp.max(s_b, 0, keepdims=True))
        e_n = jnp.exp(s_n - m_n)
        e_f = jnp.exp(s_f - m_f)
        e_b = jnp.exp(s_b - m_f)
        l_n = jnp.sum(e_n, 0, keepdims=True)
        l_f = jnp.sum(e_f, 0, keepdims=True) + jnp.sum(e_b, 0, keepdims=True)
        lse_ref[0, h : h + 1, :half] = m_n + jnp.log(l_n)
        lse_ref[0, h : h + 1, half:] = m_f + jnp.log(l_f)
        r_n, r_f = 1.0 / l_n, 1.0 / l_f
        o_n = mm(v_t[:, :length], (e_n * r_n).astype(BF))
        o_f = mm(v_t[:, :length], (e_f * r_f).astype(BF)) + mm(v_t[:, length:], (e_b * r_f).astype(BF))
        o = jnp.concatenate([o_n.T, o_f.T], 0).astype(BF)
        for j in range(count_s):
            attn_ref[me_s ^ j, 0, :, lanes] = o[j * own : (j + 1) * own]


def attn_grad_kernel(ids_ref, qb_ref, q_ref, kv_ref, do_ref, attn_ref, lse_ref, gain_ref, cos_ref, sin_ref, gq_ref, dkv_ref, gain_out, q_nat, k_nat, v_nat, do_nat, attn_nat, dk_acc, dv_acc):
    me_s, me_c = ids_ref[0], ids_ref[1]
    count_s, _, own, width = q_ref.shape
    count_c = kv_ref.shape[0]
    dim = gain_ref.shape[-1]
    rows = count_s * own
    half = rows // 2
    length = count_c * half
    scale = dim ** (-0.5)
    natural_rows(me_s, count_s, q_ref, q_nat)
    natural_rows(me_s, count_s, do_ref, do_nat)
    natural_rows(me_s, count_s, attn_ref, attn_nat)
    gather_keys(me_s, me_c, kv_ref, k_nat, v_nat)
    near, far = masks(me_c, count_c, half)
    k_t = k_nat[...].astype(F32).T.astype(BF)
    heads = width // dim
    lane = lax.broadcasted_iota(jnp.int32, (rows, dim), 1)
    delta = jnp.zeros((rows, dim), F32)
    for h in range(heads):
        lanes = slice(h * dim, (h + 1) * dim)
        both = jnp.sum(do_nat[:, lanes].astype(F32) * attn_nat[:, lanes].astype(F32), -1, keepdims=True)
        delta = jnp.where(lane == h, both, delta)
    delta_t = delta.T
    gain_total = jnp.zeros((1, dim), F32)
    for h in range(heads):
        lanes = slice(h * dim, (h + 1) * dim)
        q = qb_ref[0, :, lanes]
        do = do_nat[:, lanes]
        lse = lse_ref[0, h : h + 1, :]
        dlt = delta_t[h : h + 1, :]
        s_a = mm_nt(k_nat[:length], q) * scale
        dp_a = mm_nt(v_nat[:length], do)
        p_n = jnp.exp(jnp.where(near, s_a[:, :half], -1e30) - lse[:, :half])
        p_f = jnp.exp(s_a[:, half:] - lse[:, half:])
        p_a = jnp.concatenate([p_n, p_f], 1)
        ds_a = (p_a * (dp_a - dlt) * scale).astype(BF)
        p_a = p_a.astype(BF)
        s_b = jnp.where(far, mm_nt(k_nat[length:], q[half:]) * scale, -1e30)
        dp_b = mm_nt(v_nat[length:], do[half:])
        p_b = jnp.exp(s_b - lse[:, half:])
        ds_b = (p_b * (dp_b - dlt[:, half:]) * scale).astype(BF)
        p_b = p_b.astype(BF)
        dk_a, dv_a = mm(ds_a, q), mm(p_a, do)
        dk_b, dv_b = mm(ds_b, q[half:]), mm(p_b, do[half:])
        if h == 0:
            dk_acc[:length], dv_acc[:length] = dk_a, dv_a
            dk_acc[length:], dv_acc[length:] = dk_b, dv_b
        else:
            dk_acc[:length] += dk_a
            dv_acc[:length] += dv_a
            dk_acc[length:] += dk_b
            dv_acc[length:] += dv_b
        dq_a = mm(k_t[:, :length], ds_a)
        dq_f = dq_a[:, half:] + mm(k_t[:, length:], ds_b)
        dq = jnp.concatenate([dq_a[:, :half].T, dq_f.T], 0)
        grad = turn_back(dq, cos_ref[...], sin_ref[...])
        u = q_nat[:, lanes]
        inverse = inv_rms(u)
        hat = u * inverse
        gain_total = gain_total + jnp.sum(grad * hat, 0, keepdims=True)
        out = norm_backward_step(grad, hat, inverse, gain_ref[...]).astype(BF)
        for j in range(count_s):
            gq_ref[me_s ^ j, 0, :, lanes] = out[j * own : (j + 1) * own]
    gain_out[0] = gain_total
    for jc in range(count_c):
        for j in range(count_s):
            row = j * own
            at = jc * half + row if row < half else (2 * count_c - 1 - jc) * half + row - half
            dkv_ref[me_c ^ jc, 0, me_s ^ j, 0] = dk_acc[at : at + own, :].astype(BF)
            dkv_ref[me_c ^ jc, 1, me_s ^ j, 0] = dv_acc[at : at + own, :].astype(BF)


def expert_grad_kernel(rows_ref, grad_in_ref, grads_ref, inner_ref, out_ref):
    wide = grads_ref.shape[1]
    out_ref[:, :wide] = mm_tn(rows_ref[...], grads_ref[...]).astype(BF)
    out_ref[:, wide:] = mm_tn(grad_in_ref[...], inner_ref[...]).astype(BF)


def expert_grads(rows, grad_in, grads, inner):
    count, width = rows.shape
    tile = 256 if width % 256 == 0 else width
    wide = grads.shape[1] + inner.shape[1]

    def resident(value):
        return pl.BlockSpec(value.shape, lambda i: (0, 0))

    return pl.pallas_call(
        expert_grad_kernel,
        grid=(width // tile,),
        in_specs=[
            pl.BlockSpec((count, tile), lambda i: (0, i)),
            pl.BlockSpec((count, tile), lambda i: (0, i)),
            resident(grads),
            resident(inner),
        ],
        out_specs=pl.BlockSpec((tile, wide), lambda i: (i, 0)),
        out_shape=jax.ShapeDtypeStruct((width, wide), BF),
        name="expert_grads",
        cost_estimate=pl.CostEstimate(
            flops=2 * count * width * wide, bytes_accessed=4 * (count + wide) * width, transcendentals=0
        ),
    )(rows, grad_in, grads, inner)


def after(value, *others):
    return lax.optimization_barrier((value, *others))[0]


def per_device(
    tokens,
    gain_attn,
    gain_mlp,
    gain_query,
    key_norm_gain,
    w_query,
    key_matrix,
    value_matrix,
    w_out,
    w_gate,
    w_up,
    w_down,
    expert_ids,
    route_weight,
    cotangent,
):
    count_c = lax.axis_size("ctx")
    count_s = lax.axis_size("shard")
    me_c = lax.axis_index("ctx")
    me_s = lax.axis_index("shard")
    seqs, block_rows, width = tokens.shape
    own = expert_ids.shape[1]
    head_dim = gain_query.shape[0]
    q_width = w_query.shape[1]
    heads = q_width // head_dim
    hidden_width = w_gate.shape[2]
    half = block_rows // 2
    seq_len = block_rows * count_c
    own_rows = seqs * own
    all_rows = count_s * own_rows
    both = ("ctx", "dp")

    def gather(value):
        return lax.all_gather(value, both, axis=0, tiled=True)

    def scatter(value):
        return lax.psum_scatter(value, both, scatter_dimension=0, tiled=True)

    def sum_cores(value):
        count_d = lax.axis_size("dp")
        me_d = lax.axis_index("dp")
        parts = value.reshape(count_c, count_d, -1, value.shape[1])
        total = lax.dynamic_index_in_dim(parts, me_d, 1, False).astype(F32)
        for k in range(1, count_d):
            sent = lax.dynamic_index_in_dim(parts, me_d ^ k, 1, False)
            total = total + swap(sent, "dp", k).astype(F32)
        return total.astype(BF)

    def sum_ctx(total):
        result = lax.dynamic_index_in_dim(total, me_c, 0, False).astype(F32)
        for k in order_of(count_c):
            sent = lax.dynamic_index_in_dim(total, me_c ^ k, 0, False)
            result = result + swap(sent, "ctx", k).astype(F32)
        return result

    full_qkv = gather(jnp.concatenate([w_query, key_matrix, value_matrix], 1))
    full_out = gather(w_out)
    full_experts = gather(jnp.concatenate([w_gate[0], w_up[0], w_down[0]], 1))

    rows_at = [
        lax.dynamic_slice_in_dim(tokens, (me_s ^ k) * own, own, 1).reshape(own_rows, width)
        for k in range(count_s)
    ]
    residual = jnp.concatenate(rows_at, 0).astype(F32)
    inverse_one = inv_rms(residual)
    hat_one = residual * inverse_one
    normed_one = (hat_one * gain_attn).astype(BF)
    residual_own = rows_at[0].astype(F32)
    inverse_own = inv_rms(residual_own)
    hat_own = residual_own * inverse_own

    grad_top = cotangent.reshape(own_rows, width)
    grad_all = jnp.concatenate(collect(grad_top, "shard"), 0)
    ids = expert_ids.reshape(own_rows, -1)
    weights = route_weight.reshape(own_rows, -1)

    def weight_for(expert):
        return jnp.sum(jnp.where(ids == expert, weights, 0.0), -1)

    coefs = {0: weight_for(me_s)}
    for k in order_of(count_s):
        coefs[k] = swap(weight_for(me_s ^ k), "shard", k)
    coef = jnp.concatenate([coefs[k] for k in range(count_s)], 0)[:, None]
    grad_rows = (coef * grad_all.astype(F32)).astype(BF)

    block = jnp.arange(count_s, dtype=jnp.int32)
    offsets = jnp.arange(own, dtype=jnp.int32)
    row_natural = me_c * block_rows + jnp.arange(block_rows, dtype=jnp.int32)
    cos_nat, sin_nat = rope_tables(folded_positions(row_natural, count_c, half), head_dim)
    row_peer = me_c * block_rows + (me_s ^ block)[:, None] * own + offsets
    cos_peer, sin_peer = rope_tables(folded_positions(row_peer, count_c, half), head_dim)

    def spread(table):
        return jnp.broadcast_to(
            table[:, None], (count_s, seqs, own, head_dim)
        ).reshape(all_rows, head_dim)

    cos_rows, sin_rows = spread(cos_peer), spread(sin_peer)
    gain_q_row, gain_k_row = gain_query[None], key_norm_gain[None]

    normed_one = after(normed_one, grad_rows)
    kv_raw = mm(normed_one, full_qkv[:, q_width:])
    kv_own = pl.pallas_call(
        key_kernel, out_shape=jax.ShapeDtypeStruct((2, all_rows, head_dim), BF), name="key_prep"
    )(kv_raw, gain_k_row, cos_rows, sin_rows)
    kv_all = jnp.stack(collect(kv_own, "ctx"), 0).reshape(
        count_c, 2, count_s, seqs, own, head_dim
    )
    full_query = lax.optimization_barrier(full_qkv[:, :q_width])
    queries = mm(normed_one, full_query).reshape(count_s, seqs, own, q_width)
    kv_weights = jnp.concatenate(collect(full_qkv[:, q_width:], "shard"), 1)

    me_ids = jnp.stack([me_s, me_c]).astype(jnp.int32)
    row_spec = pl.BlockSpec((count_s, 1, own, q_width), lambda s, _: (0, s, 0, 0))
    kv_spec = pl.BlockSpec(
        (count_c, 2, count_s, 1, own, head_dim), lambda s, _: (0, 0, 0, s, 0, 0)
    )
    nat_spec = pl.BlockSpec((1, block_rows, q_width), lambda s, _: (s, 0, 0))
    lse_spec = pl.BlockSpec((1, heads, block_rows), lambda s, _: (s, 0, 0))

    def whole(shape):
        return pl.BlockSpec(shape, lambda s, _: (0,) * len(shape))

    table_spec = whole((block_rows, head_dim))
    gain_spec = whole((1, head_dim))
    me_ids, kv_weights = lax.optimization_barrier((me_ids, kv_weights))
    attn, lse, queries_bf = pl.pallas_call(
        attn_kernel,
        grid_spec=pltpu.PrefetchScalarGridSpec(
            num_scalar_prefetch=1,
            grid=(seqs,),
            in_specs=[row_spec, kv_spec, gain_spec, table_spec, table_spec],
            out_specs=[row_spec, lse_spec, nat_spec],
            scratch_shapes=[
                pltpu.VMEM((block_rows, q_width), F32),
                pltpu.VMEM((seq_len, head_dim), BF),
                pltpu.VMEM((seq_len, head_dim), BF),
            ],
        ),
        out_shape=[
            jax.ShapeDtypeStruct((count_s, seqs, own, q_width), BF),
            jax.ShapeDtypeStruct((seqs, heads, block_rows), F32),
            jax.ShapeDtypeStruct((seqs, block_rows, q_width), BF),
        ],
        name="attn_fwd",
        cost_estimate=pl.CostEstimate(
            flops=4 * all_rows * seq_len * q_width, bytes_accessed=16 * all_rows * q_width, transcendentals=0
        ),
    )(me_ids, queries, kv_all, gain_q_row, cos_nat, sin_nat)

    half_width = width // 2
    sides = (slice(0, half_width), slice(half_width, width))

    def reduce_blocks(term, crossed):
        def send(value, k):
            return swap(value.astype(BF), "shard", k)

        low, high = sides
        if count_s != 4 or not crossed:
            full = slice(0, width)
            got = {k: send(term(k, full), k) for k in order_of(count_s)}
            total = term(0, full).astype(F32)
            for part in got.values():
                total = total + part.astype(F32)
            return total
        far_low = send(term(3, low), 1)
        far_high = send(term(3, high), 2)
        near_low = send(term(1, low), 1)
        near_high = send(term(2, high), 2)
        relay_low = swap((term(2, low).astype(F32) + far_low.astype(F32)).astype(BF), "shard", 2)
        relay_high = swap((term(1, high).astype(F32) + far_high.astype(F32)).astype(BF), "shard", 1)
        total_low = term(0, low).astype(F32) + near_low.astype(F32) + relay_low.astype(F32)
        total_high = term(0, high).astype(F32) + near_high.astype(F32) + relay_high.astype(F32)
        return jnp.concatenate([total_low, total_high], 1)

    def block_rows_of(value):
        return lambda k, columns: value[k * own_rows : (k + 1) * own_rows, columns]

    attended = reduce_blocks(
        lambda k, columns: mm_nt(attn[k].reshape(own_rows, q_width), full_out[columns]), True
    )
    hidden = residual_own + attended
    inverse_two = inv_rms(hidden)
    hat_two = hidden * inverse_two
    normed_two = (hat_two * gain_mlp).astype(BF)
    arrived = collect_crossed(normed_two, "shard")

    full_gate_up = full_experts[:, : 2 * hidden_width]
    full_down = full_experts[:, 2 * hidden_width :]
    grad_inner = mm(grad_rows, full_down)
    pre = mm(arrived, full_gate_up)
    gate_pre, up_pre = pre[:, :hidden_width], pre[:, hidden_width:]
    gate_sig = jax.nn.sigmoid(gate_pre)
    gate_act = gate_pre * gate_sig
    inner_bf = (gate_act * up_pre).astype(BF)
    grad_gate = grad_inner * up_pre * gate_sig * (1.0 + gate_pre * (1.0 - gate_sig))
    grad_up = grad_inner * gate_act
    grad_gate_up = jnp.concatenate([grad_gate.astype(BF), grad_up.astype(BF)], 1)
    grad_slots = mm_nt(grad_gate_up, full_gate_up)
    grad_normed_two = reduce_blocks(block_rows_of(grad_slots.astype(BF)), True)
    grad_w_experts = expert_grads(arrived, grad_rows, after(grad_gate_up, grad_slots), inner_bf)
    sum_experts = scatter(grad_w_experts).astype(F32)

    gain_mlp_part = jnp.sum(grad_normed_two * hat_two, 0)
    grad_hidden = grad_top.astype(F32) + norm_backward_step(
        grad_normed_two, hat_two, inverse_two, gain_mlp
    )
    expert_out = mm_nt(inner_bf, full_down).astype(BF).astype(F32)
    weighted = coef * expert_out
    weighted = weighted.astype(BF)
    route_part = jnp.sum(grad_all.astype(F32) * expert_out, -1)
    grad_hidden_bf = after(grad_hidden.astype(BF), grad_w_experts)
    grad_att = collect_crossed(grad_hidden_bf, "shard")
    grad_att, weighted = lax.optimization_barrier((grad_att, weighted))
    mixture = reduce_blocks(block_rows_of(weighted), False)
    block_out = (hidden + mixture).astype(BF)
    route_all = {0: route_part[:own_rows]}
    for k in order_of(count_s):
        route_all[k] = swap(route_part[k * own_rows : (k + 1) * own_rows], "shard", k)
    route_grad = jnp.zeros(ids.shape, F32)
    for k in range(count_s):
        route_grad = jnp.where(ids == (me_s ^ k), route_all[k][:, None], route_grad)

    attention_gradient = mm(grad_att, full_out).astype(BF)

    grad_q, grad_kv, gain_q_parts = pl.pallas_call(
        attn_grad_kernel,
        grid_spec=pltpu.PrefetchScalarGridSpec(
            num_scalar_prefetch=1,
            grid=(seqs,),
            in_specs=[
                nat_spec, row_spec, kv_spec, row_spec, row_spec, lse_spec,
                gain_spec, table_spec, table_spec,
            ],
            out_specs=[row_spec, kv_spec, pl.BlockSpec((1, 1, head_dim), lambda s, _: (s, 0, 0))],
            scratch_shapes=[
                pltpu.VMEM((block_rows, q_width), F32),
                pltpu.VMEM((seq_len, head_dim), BF),
                pltpu.VMEM((seq_len, head_dim), BF),
                pltpu.VMEM((block_rows, q_width), BF),
                pltpu.VMEM((block_rows, q_width), BF),
                pltpu.VMEM((seq_len, head_dim), F32),
                pltpu.VMEM((seq_len, head_dim), F32),
            ],
        ),
        out_shape=[
            jax.ShapeDtypeStruct((count_s, seqs, own, q_width), BF),
            jax.ShapeDtypeStruct((count_c, 2, count_s, seqs, own, head_dim), BF),
            jax.ShapeDtypeStruct((seqs, 1, head_dim), F32),
        ],
        name="attn_bwd",
        cost_estimate=pl.CostEstimate(
            flops=10 * all_rows * seq_len * q_width, bytes_accessed=32 * all_rows * q_width, transcendentals=0
        ),
    )(
        me_ids, queries_bf, queries, kv_all,
        attention_gradient.reshape(count_s, seqs, own, q_width),
        attn, lse, gain_q_row, cos_nat, sin_nat,
    )
    grad_kv = grad_kv.reshape(count_c, 2, all_rows, head_dim)
    grad_q = grad_q.reshape(all_rows, q_width)
    grad_w_query = mm_tn(normed_one, grad_q).astype(BF)
    sum_query = scatter(grad_w_query).astype(F32)
    query_part = reduce_blocks(
        lambda k, columns: mm_nt(grad_q[k * own_rows : (k + 1) * own_rows], full_query[columns]),
        False,
    )
    grad_w_out = mm_tn(after(grad_att, grad_kv), attn.reshape(all_rows, q_width)).astype(BF)
    half_sum_out = sum_cores(grad_w_out)
    sum_out = sum_ctx(half_sum_out)

    kv_parts = [grad_kv[0]]
    for k in range(1, count_c):
        kv_parts.append(swap(grad_kv[k], "ctx", k))
    kv_parts = list(lax.optimization_barrier((*kv_parts, half_sum_out))[:count_c])
    grad_kv_bf, gain_k_part = pl.pallas_call(
        functools.partial(key_grad_kernel, count_c),
        out_shape=[
            jax.ShapeDtypeStruct((all_rows, 2 * head_dim), BF),
            jax.ShapeDtypeStruct((1, head_dim), F32),
        ],
        name="key_grad",
    )(kv_raw, gain_k_row, cos_rows, sin_rows, *kv_parts)
    kv_rows = {
        k: swap(grad_kv_bf[k * own_rows : (k + 1) * own_rows], "shard", k)
        for k in order_of(count_s)
    }
    kv_rows[0] = grad_kv_bf[:own_rows]
    half_sum_kv = sum_cores(mm_tn(normed_one, grad_kv_bf).astype(BF))
    sum_kv = sum_ctx(half_sum_kv)
    kv_all_rows = jnp.concatenate([kv_rows[k] for k in range(count_s)], 1)
    kv_all_rows = after(kv_all_rows, half_sum_kv)
    grad_normed_one = query_part + mm_nt(kv_all_rows, kv_weights)
    gain_attn_part = jnp.sum(grad_normed_one * hat_own, 0)
    grad_tokens = grad_hidden + norm_backward_step(
        grad_normed_one, hat_own, inverse_own, gain_attn
    )
    gains = jnp.concatenate(
        [gain_attn_part, gain_mlp_part, jnp.sum(gain_q_parts, (0, 1)), gain_k_part[0]]
    ).reshape(-1, head_dim)
    for axis in ("dp", "shard", "ctx"):
        step = 1
        while step < lax.axis_size(axis):
            gains = gains + swap(gains, axis, step)
            step *= 2
        if axis == "shard":
            gains, sum_experts = lax.optimization_barrier((gains, sum_experts))
    gains = gains.reshape(-1)

    def own_shape(value):
        return value.reshape(seqs, own, value.shape[-1])

    return (
        own_shape(block_out),
        own_shape(grad_tokens),
        lse,
        own_shape(route_grad),
        gains[:width],
        gains[width : 2 * width],
        gains[2 * width : 2 * width + head_dim],
        gains[2 * width + head_dim :],
        sum_query,
        sum_kv[:, :head_dim],
        sum_kv[:, head_dim:],
        sum_out,
        sum_experts[None, :, :hidden_width],
        sum_experts[None, :, hidden_width : 2 * hidden_width],
        sum_experts[None, :, 2 * hidden_width :],
    )


def solution(mesh):
    placed = (
        P("dp", "ctx", None),
        P(),
        P(),
        P(),
        P(),
        P(("ctx", "dp"), "shard"),
        P(("ctx", "dp"), "shard"),
        P(("ctx", "dp"), "shard"),
        P(("ctx", "dp"), "shard"),
        P("shard", ("ctx", "dp"), None),
        P("shard", ("ctx", "dp"), None),
        P("shard", ("ctx", "dp"), None),
        P("dp", ("ctx", "shard"), None),
        P("dp", ("ctx", "shard"), None),
        P("dp", ("ctx", "shard"), None),
    )

    return jax.shard_map(
        per_device,
        mesh=mesh,
        in_specs=placed,
        out_specs=(
            P("dp", ("ctx", "shard"), None),
            P("dp", ("ctx", "shard"), None),
            P("dp", "shard", "ctx"),
            P("dp", ("ctx", "shard"), None),
            P(),
            P(),
            P(),
            P(),
            P(("ctx", "dp"), "shard"),
            P(("ctx", "dp"), "shard"),
            P(("ctx", "dp"), "shard"),
            P(("ctx", "dp"), "shard"),
            P("shard", ("ctx", "dp"), None),
            P("shard", ("ctx", "dp"), None),
            P("shard", ("ctx", "dp"), None),
        ),
        check_vma=False,
    )
```

```python
import functools

import jax
import jax.numpy as jnp
from jax import lax
from jax.experimental import pallas as pl
from jax.experimental.pallas import tpu as pltpu
from jax.sharding import PartitionSpec as P


epsilon = 1e-06
theta_base = 1000000.0
BF = jnp.bfloat16
F32 = jnp.float32


def pairs(count, k):
    return [(i, i ^ k) for i in range(count)]


def swap(value, axis, k):
    return lax.ppermute(value, axis, pairs(lax.axis_size(axis), k))


def order_of(count):
    return sorted(range(1, count), key=lambda k: -bin(k).count("1"))


def collect(value, axis):
    count = lax.axis_size(axis)
    got = {0: value}
    for k in order_of(count):
        got[k] = swap(value, axis, k)
    return [got[k] for k in range(count)]


def join_kernel(*refs):
    *parts, out_ref = refs
    rows, half = parts[0].shape
    for k in range(len(parts) // 2):
        out_ref[k * rows : (k + 1) * rows, :half] = parts[2 * k][...]
        out_ref[k * rows : (k + 1) * rows, half:] = parts[2 * k + 1][...]


def join(parts):
    rows, half = parts[0].shape
    shape = (len(parts) // 2 * rows, 2 * half)
    return pl.pallas_call(
        join_kernel,
        out_shape=jax.ShapeDtypeStruct(shape, parts[0].dtype),
        name="join",
        cost_estimate=pl.CostEstimate(
            flops=0, bytes_accessed=4 * shape[0] * shape[1], transcendentals=0
        ),
    )(*parts)


def collect_crossed(value, axis, *others):
    if lax.axis_size(axis) != 4:
        return after(jnp.concatenate(collect(value, axis), 0), *others)
    half = value.shape[1] // 2
    low, high = value[:, :half], value[:, half:]

    def send(part, k):
        return swap(part, axis, k)

    low_1, high_2 = send(low, 1), send(high, 2)
    high_1, low_2 = send(high, 1), send(low, 2)
    low_3, high_3 = swap(low_1, axis, 2), swap(high_2, axis, 1)
    parts = (low, high, low_1, high_1, low_2, high_2, low_3, high_3)
    return join(lax.optimization_barrier((*parts, *others))[: len(parts)])


def folded_positions(rows, count_ctx, half_block):
    block = rows // half_block
    offset = rows % half_block
    device = block // 2
    placed = jnp.where(block % 2 == 0, device, 2 * count_ctx - 1 - device)
    return placed * half_block + offset


def rope_tables(positions, head_dim):
    freq = jnp.arange(head_dim // 2, dtype=F32) * (2.0 / head_dim)
    inverse = jnp.power(jnp.float32(theta_base), -freq)
    angles = positions.astype(F32)[..., None] * inverse
    cosine, sine = jnp.cos(angles), jnp.sin(angles)
    return jnp.concatenate([cosine, cosine], -1), jnp.concatenate([-sine, sine], -1)


def inv_rms(field):
    return lax.rsqrt(jnp.mean(field * field, -1, keepdims=True) + epsilon)


def norm_backward_step(grad_normed, normed_hat, inverse, gain):
    scaled = grad_normed * gain
    return inverse * (scaled - normed_hat * jnp.mean(scaled * normed_hat, -1, keepdims=True))


def mm(a, b):
    return lax.dot_general(a, b, (((1,), (0,)), ((), ())), preferred_element_type=F32)


def mm_nt(a, b):
    return lax.dot_general(a, b, (((1,), (1,)), ((), ())), preferred_element_type=F32)


def mm_tn(a, b):
    return lax.dot_general(a, b, (((0,), (0,)), ((), ())), preferred_element_type=F32)


def turn(u, cosine, sine):
    return u * cosine + pltpu.roll(u, u.shape[-1] // 2, 1) * sine


def turn_back(u, cosine, sine):
    return u * cosine - pltpu.roll(u, u.shape[-1] // 2, 1) * sine


def key_kernel(raw_ref, gain_ref, cos_ref, sin_ref, out_ref):
    dim = gain_ref.shape[-1]
    raw = raw_ref[:, :dim]
    unit = raw * inv_rms(raw)
    out_ref[0] = turn(unit * gain_ref[...], cos_ref[...], sin_ref[...]).astype(BF)
    out_ref[1] = raw_ref[:, dim:].astype(BF)


def key_grad_kernel(count, raw_ref, gain_ref, cos_ref, sin_ref, *refs):
    parts, (out_ref, gain_out) = refs[:count], refs[count:]
    dim = gain_ref.shape[-1]
    total = parts[0][...].astype(F32)
    for part in parts[1:]:
        total = total + part[...].astype(F32)
    raw = raw_ref[:, :dim]
    inverse = inv_rms(raw)
    unit = raw * inverse
    grad = turn_back(total[0], cos_ref[...], sin_ref[...])
    gain_out[...] = jnp.sum(grad * unit, 0, keepdims=True)
    out_ref[:, :dim] = norm_backward_step(grad, unit, inverse, gain_ref[...]).astype(BF)
    out_ref[:, dim:] = total[1].astype(BF)


def natural_rows(me_s, count_s, ref, out_ref):
    own = out_ref.shape[0] // count_s
    for j in range(count_s):
        out_ref[j * own : (j + 1) * own, :] = ref[me_s ^ j, 0]


def gather_keys(me_s, me_c, kv_ref, k_nat, v_nat):
    count_c, _, count_s, _, own, _ = kv_ref.shape
    half = count_s * own // 2
    for jc in range(count_c):
        for j in range(count_s):
            row = j * own
            at = jc * half + row if row < half else (2 * count_c - 1 - jc) * half + row - half
            k_nat[at : at + own, :] = kv_ref[me_c ^ jc, 0, me_s ^ j, 0]
            v_nat[at : at + own, :] = kv_ref[me_c ^ jc, 1, me_s ^ j, 0]


def masks(me_c, count_c, half):
    length = count_c * half
    key = lax.broadcasted_iota(jnp.int32, (length, half), 0)
    lane = lax.broadcasted_iota(jnp.int32, (length, half), 1)
    near = key <= me_c * half + lane
    far = key + length <= (2 * count_c - 1 - me_c) * half + lane
    return near, far


def attn_kernel(ids_ref, q_ref, kv_ref, gain_ref, cos_ref, sin_ref, attn_ref, lse_ref, qb_ref, q_nat, k_nat, v_nat):
    me_s, me_c = ids_ref[0], ids_ref[1]
    count_s, _, own, width = q_ref.shape
    count_c = kv_ref.shape[0]
    dim = gain_ref.shape[-1]
    rows = count_s * own
    half = rows // 2
    length = count_c * half
    scale = dim ** (-0.5)
    natural_rows(me_s, count_s, q_ref, q_nat)
    gather_keys(me_s, me_c, kv_ref, k_nat, v_nat)
    near, far = masks(me_c, count_c, half)
    v_t = v_nat[...].astype(F32).T.astype(BF)
    for h in range(width // dim):
        lanes = slice(h * dim, (h + 1) * dim)
        u = q_nat[:, lanes]
        q = turn(u * inv_rms(u) * gain_ref[...], cos_ref[...], sin_ref[...]).astype(BF)
        qb_ref[0, :, lanes] = q
        s_a = mm_nt(k_nat[:length], q) * scale
        s_n = jnp.where(near, s_a[:, :half], -1e30)
        s_f = s_a[:, half:]
        s_b = jnp.where(far, mm_nt(k_nat[length:], q[half:]) * scale, -1e30)
        m_n = jnp.max(s_n, 0, keepdims=True)
        m_f = jnp.maximum(jnp.max(s_f, 0, keepdims=True), jnp.max(s_b, 0, keepdims=True))
        e_n = jnp.exp(s_n - m_n)
        e_f = jnp.exp(s_f - m_f)
        e_b = jnp.exp(s_b - m_f)
        l_n = jnp.sum(e_n, 0, keepdims=True)
        l_f = jnp.sum(e_f, 0, keepdims=True) + jnp.sum(e_b, 0, keepdims=True)
        lse_ref[0, h : h + 1, :half] = m_n + jnp.log(l_n)
        lse_ref[0, h : h + 1, half:] = m_f + jnp.log(l_f)
        r_n, r_f = 1.0 / l_n, 1.0 / l_f
        o_n = mm(v_t[:, :length], (e_n * r_n).astype(BF))
        o_f = mm(v_t[:, :length], (e_f * r_f).astype(BF)) + mm(v_t[:, length:], (e_b * r_f).astype(BF))
        o = jnp.concatenate([o_n.T, o_f.T], 0).astype(BF)
        for j in range(count_s):
            attn_ref[me_s ^ j, 0, :, lanes] = o[j * own : (j + 1) * own]


def attn_grad_kernel(ids_ref, qb_ref, q_ref, kv_ref, do_ref, attn_ref, lse_ref, gain_ref, cos_ref, sin_ref, gq_ref, dkv_ref, gain_out, q_nat, k_nat, v_nat, do_nat, attn_nat, dk_acc, dv_acc):
    me_s, me_c = ids_ref[0], ids_ref[1]
    count_s, _, own, width = q_ref.shape
    count_c = kv_ref.shape[0]
    dim = gain_ref.shape[-1]
    rows = count_s * own
    half = rows // 2
    length = count_c * half
    scale = dim ** (-0.5)
    natural_rows(me_s, count_s, q_ref, q_nat)
    natural_rows(me_s, count_s, do_ref, do_nat)
    natural_rows(me_s, count_s, attn_ref, attn_nat)
    gather_keys(me_s, me_c, kv_ref, k_nat, v_nat)
    near, far = masks(me_c, count_c, half)
    k_t = k_nat[...].astype(F32).T.astype(BF)
    heads = width // dim
    lane = lax.broadcasted_iota(jnp.int32, (rows, dim), 1)
    delta = jnp.zeros((rows, dim), F32)
    for h in range(heads):
        lanes = slice(h * dim, (h + 1) * dim)
        both = jnp.sum(do_nat[:, lanes].astype(F32) * attn_nat[:, lanes].astype(F32), -1, keepdims=True)
        delta = jnp.where(lane == h, both, delta)
    delta_t = delta.T
    gain_total = jnp.zeros((1, dim), F32)
    for h in range(heads):
        lanes = slice(h * dim, (h + 1) * dim)
        q = qb_ref[0, :, lanes]
        do = do_nat[:, lanes]
        lse = lse_ref[0, h : h + 1, :]
        dlt = delta_t[h : h + 1, :]
        s_a = mm_nt(k_nat[:length], q) * scale
        dp_a = mm_nt(v_nat[:length], do)
        p_n = jnp.exp(jnp.where(near, s_a[:, :half], -1e30) - lse[:, :half])
        p_f = jnp.exp(s_a[:, half:] - lse[:, half:])
        p_a = jnp.concatenate([p_n, p_f], 1)
        ds_a = (p_a * (dp_a - dlt) * scale).astype(BF)
        p_a = p_a.astype(BF)
        s_b = jnp.where(far, mm_nt(k_nat[length:], q[half:]) * scale, -1e30)
        dp_b = mm_nt(v_nat[length:], do[half:])
        p_b = jnp.exp(s_b - lse[:, half:])
        ds_b = (p_b * (dp_b - dlt[:, half:]) * scale).astype(BF)
        p_b = p_b.astype(BF)
        dk_a, dv_a = mm(ds_a, q), mm(p_a, do)
        dk_b, dv_b = mm(ds_b, q[half:]), mm(p_b, do[half:])
        if h == 0:
            dk_acc[:length], dv_acc[:length] = dk_a, dv_a
            dk_acc[length:], dv_acc[length:] = dk_b, dv_b
        else:
            dk_acc[:length] += dk_a
            dv_acc[:length] += dv_a
            dk_acc[length:] += dk_b
            dv_acc[length:] += dv_b
        dq_a = mm(k_t[:, :length], ds_a)
        dq_f = dq_a[:, half:] + mm(k_t[:, length:], ds_b)
        dq = jnp.concatenate([dq_a[:, :half].T, dq_f.T], 0)
        grad = turn_back(dq, cos_ref[...], sin_ref[...])
        u = q_nat[:, lanes]
        inverse = inv_rms(u)
        hat = u * inverse
        gain_total = gain_total + jnp.sum(grad * hat, 0, keepdims=True)
        out = norm_backward_step(grad, hat, inverse, gain_ref[...]).astype(BF)
        for j in range(count_s):
            gq_ref[me_s ^ j, 0, :, lanes] = out[j * own : (j + 1) * own]
    gain_out[0] = gain_total
    for jc in range(count_c):
        for j in range(count_s):
            row = j * own
            at = jc * half + row if row < half else (2 * count_c - 1 - jc) * half + row - half
            dkv_ref[me_c ^ jc, 0, me_s ^ j, 0] = dk_acc[at : at + own, :].astype(BF)
            dkv_ref[me_c ^ jc, 1, me_s ^ j, 0] = dv_acc[at : at + own, :].astype(BF)


def expert_grad_kernel(rows_ref, grad_in_ref, grads_ref, inner_ref, out_ref):
    wide = grads_ref.shape[1]
    out_ref[:, :wide] = mm_tn(rows_ref[...], grads_ref[...]).astype(BF)
    out_ref[:, wide:] = mm_tn(grad_in_ref[...], inner_ref[...]).astype(BF)


def expert_grads(rows, grad_in, grads, inner):
    count, width = rows.shape
    tile = 256 if width % 256 == 0 else width
    wide = grads.shape[1] + inner.shape[1]

    def resident(value):
        return pl.BlockSpec(value.shape, lambda i: (0, 0))

    return pl.pallas_call(
        expert_grad_kernel,
        grid=(width // tile,),
        in_specs=[
            pl.BlockSpec((count, tile), lambda i: (0, i)),
            pl.BlockSpec((count, tile), lambda i: (0, i)),
            resident(grads),
            resident(inner),
        ],
        out_specs=pl.BlockSpec((tile, wide), lambda i: (i, 0)),
        out_shape=jax.ShapeDtypeStruct((width, wide), BF),
        name="expert_grads",
        cost_estimate=pl.CostEstimate(
            flops=2 * count * width * wide, bytes_accessed=4 * (count + wide) * width, transcendentals=0
        ),
    )(rows, grad_in, grads, inner)


def after(value, *others):
    return lax.optimization_barrier((value, *others))[0]


def per_device(
    tokens,
    gain_attn,
    gain_mlp,
    gain_query,
    key_norm_gain,
    w_query,
    key_matrix,
    value_matrix,
    w_out,
    w_gate,
    w_up,
    w_down,
    expert_ids,
    route_weight,
    cotangent,
):
    count_c = lax.axis_size("ctx")
    count_s = lax.axis_size("shard")
    me_c = lax.axis_index("ctx")
    me_s = lax.axis_index("shard")
    seqs, block_rows, width = tokens.shape
    own = expert_ids.shape[1]
    head_dim = gain_query.shape[0]
    q_width = w_query.shape[1]
    heads = q_width // head_dim
    hidden_width = w_gate.shape[2]
    half = block_rows // 2
    seq_len = block_rows * count_c
    own_rows = seqs * own
    all_rows = count_s * own_rows
    both = ("ctx", "dp")

    def gather(value):
        return lax.all_gather(value, both, axis=0, tiled=True)

    def scatter(value):
        return lax.psum_scatter(value, both, scatter_dimension=0, tiled=True)

    def sum_cores(value):
        count_d = lax.axis_size("dp")
        me_d = lax.axis_index("dp")
        parts = value.reshape(count_c, count_d, -1, value.shape[1])
        total = lax.dynamic_index_in_dim(parts, me_d, 1, False).astype(F32)
        for k in range(1, count_d):
            sent = lax.dynamic_index_in_dim(parts, me_d ^ k, 1, False)
            total = total + swap(sent, "dp", k).astype(F32)
        return total.astype(BF)

    def sum_ctx(total, *others):
        result = lax.dynamic_index_in_dim(total, me_c, 0, False).astype(F32)
        parts = []
        for k in order_of(count_c):
            sent = lax.dynamic_index_in_dim(total, me_c ^ k, 0, False)
            parts.append(swap(sent, "ctx", k))
        parts = lax.optimization_barrier((*parts, *others))[: len(parts)]
        for part in parts:
            result = result + part.astype(F32)
        return result

    full_qkv = gather(jnp.concatenate([w_query, key_matrix, value_matrix], 1))
    full_out = gather(w_out)
    full_experts = gather(jnp.concatenate([w_gate[0], w_up[0], w_down[0]], 1))

    rows_at = [
        lax.dynamic_slice_in_dim(tokens, (me_s ^ k) * own, own, 1).reshape(own_rows, width)
        for k in range(count_s)
    ]
    residual = jnp.concatenate(rows_at, 0).astype(F32)
    inverse_one = inv_rms(residual)
    hat_one = residual * inverse_one
    normed_one = (hat_one * gain_attn).astype(BF)
    residual_own = rows_at[0].astype(F32)
    inverse_own = inv_rms(residual_own)
    hat_own = residual_own * inverse_own

    grad_top = cotangent.reshape(own_rows, width)
    grad_all = jnp.concatenate(collect(grad_top, "shard"), 0)
    ids = expert_ids.reshape(own_rows, -1)
    weights = route_weight.reshape(own_rows, -1)

    def weight_for(expert):
        return jnp.sum(jnp.where(ids == expert, weights, 0.0), -1)

    coefs = {0: weight_for(me_s)}
    for k in order_of(count_s):
        coefs[k] = swap(weight_for(me_s ^ k), "shard", k)
    coef = jnp.concatenate([coefs[k] for k in range(count_s)], 0)[:, None]
    grad_rows = (coef * grad_all.astype(F32)).astype(BF)

    block = jnp.arange(count_s, dtype=jnp.int32)
    offsets = jnp.arange(own, dtype=jnp.int32)
    row_natural = me_c * block_rows + jnp.arange(block_rows, dtype=jnp.int32)
    cos_nat, sin_nat = rope_tables(folded_positions(row_natural, count_c, half), head_dim)
    row_peer = me_c * block_rows + (me_s ^ block)[:, None] * own + offsets
    cos_peer, sin_peer = rope_tables(folded_positions(row_peer, count_c, half), head_dim)

    def spread(table):
        return jnp.broadcast_to(
            table[:, None], (count_s, seqs, own, head_dim)
        ).reshape(all_rows, head_dim)

    cos_rows, sin_rows = spread(cos_peer), spread(sin_peer)
    gain_q_row, gain_k_row = gain_query[None], key_norm_gain[None]

    normed_one = after(normed_one, grad_rows)
    kv_raw = mm(normed_one, full_qkv[:, q_width:])
    kv_own = pl.pallas_call(
        key_kernel, out_shape=jax.ShapeDtypeStruct((2, all_rows, head_dim), BF), name="key_prep"
    )(kv_raw, gain_k_row, cos_rows, sin_rows)
    kv_all = jnp.stack(collect(kv_own, "ctx"), 0).reshape(
        count_c, 2, count_s, seqs, own, head_dim
    )
    full_query = lax.optimization_barrier(full_qkv[:, :q_width])
    queries = mm(normed_one, full_query).reshape(count_s, seqs, own, q_width)
    kv_weights = [full_qkv[:, q_width:]]
    for k in range(1, count_s):
        kv_weights.append(swap(kv_weights[0], "shard", k))
    kv_weights = jnp.concatenate(kv_weights, 1)

    me_ids = jnp.stack([me_s, me_c]).astype(jnp.int32)
    row_spec = pl.BlockSpec((count_s, 1, own, q_width), lambda s, _: (0, s, 0, 0))
    kv_spec = pl.BlockSpec(
        (count_c, 2, count_s, 1, own, head_dim), lambda s, _: (0, 0, 0, s, 0, 0)
    )
    nat_spec = pl.BlockSpec((1, block_rows, q_width), lambda s, _: (s, 0, 0))
    lse_spec = pl.BlockSpec((1, heads, block_rows), lambda s, _: (s, 0, 0))

    def whole(shape):
        return pl.BlockSpec(shape, lambda s, _: (0,) * len(shape))

    table_spec = whole((block_rows, head_dim))
    gain_spec = whole((1, head_dim))
    attn, lse, queries_bf = pl.pallas_call(
        attn_kernel,
        grid_spec=pltpu.PrefetchScalarGridSpec(
            num_scalar_prefetch=1,
            grid=(seqs,),
            in_specs=[row_spec, kv_spec, gain_spec, table_spec, table_spec],
            out_specs=[row_spec, lse_spec, nat_spec],
            scratch_shapes=[
                pltpu.VMEM((block_rows, q_width), F32),
                pltpu.VMEM((seq_len, head_dim), BF),
                pltpu.VMEM((seq_len, head_dim), BF),
            ],
        ),
        out_shape=[
            jax.ShapeDtypeStruct((count_s, seqs, own, q_width), BF),
            jax.ShapeDtypeStruct((seqs, heads, block_rows), F32),
            jax.ShapeDtypeStruct((seqs, block_rows, q_width), BF),
        ],
        name="attn_fwd",
        cost_estimate=pl.CostEstimate(
            flops=4 * all_rows * seq_len * q_width, bytes_accessed=16 * all_rows * q_width, transcendentals=0
        ),
    )(me_ids, queries, kv_all, gain_q_row, cos_nat, sin_nat)

    half_width = width // 2
    sides = (slice(0, half_width), slice(half_width, width))

    def reduce_blocks(term, crossed):
        def send(value, k):
            return swap(value.astype(BF), "shard", k)

        low, high = sides
        if count_s != 4 or not crossed:
            full = slice(0, width)
            got = {k: send(term(k, full), k) for k in order_of(count_s)}
            total = term(0, full).astype(F32)
            for part in got.values():
                total = total + part.astype(F32)
            return total
        far_low = send(term(3, low), 1)
        far_high = send(term(3, high), 2)
        near_low = send(term(1, low), 1)
        near_high = send(term(2, high), 2)
        relay_low = swap((term(2, low).astype(F32) + far_low.astype(F32)).astype(BF), "shard", 2)
        relay_high = swap((term(1, high).astype(F32) + far_high.astype(F32)).astype(BF), "shard", 1)
        total_low = term(0, low).astype(F32) + near_low.astype(F32) + relay_low.astype(F32)
        total_high = term(0, high).astype(F32) + near_high.astype(F32) + relay_high.astype(F32)
        return jnp.concatenate([total_low, total_high], 1)

    def block_rows_of(value):
        return lambda k, columns: value[k * own_rows : (k + 1) * own_rows, columns]

    attended = reduce_blocks(
        lambda k, columns: mm_nt(attn[k].reshape(own_rows, q_width), full_out[columns]), True
    )
    hidden = residual_own + attended
    inverse_two = inv_rms(hidden)
    hat_two = hidden * inverse_two
    normed_two = (hat_two * gain_mlp).astype(BF)
    arrived = collect_crossed(normed_two, "shard", kv_weights)

    full_gate_up = full_experts[:, : 2 * hidden_width]
    full_down = full_experts[:, 2 * hidden_width :]
    grad_inner = mm(grad_rows, full_down)
    pre = mm(arrived, full_gate_up)
    gate_pre, up_pre = pre[:, :hidden_width], pre[:, hidden_width:]
    gate_sig = jax.nn.sigmoid(gate_pre)
    gate_act = gate_pre * gate_sig
    inner_bf = (gate_act * up_pre).astype(BF)
    grad_gate = grad_inner * up_pre * gate_sig * (1.0 + gate_pre * (1.0 - gate_sig))
    grad_up = grad_inner * gate_act
    grad_gate_up = jnp.concatenate([grad_gate.astype(BF), grad_up.astype(BF)], 1)
    grad_slots = mm_nt(grad_gate_up, full_gate_up)
    grad_normed_two = reduce_blocks(block_rows_of(grad_slots.astype(BF)), True)
    grad_w_experts = expert_grads(arrived, grad_rows, after(grad_gate_up, grad_slots), inner_bf)
    sum_experts = scatter(grad_w_experts).astype(F32)

    gain_mlp_part = jnp.sum(grad_normed_two * hat_two, 0)
    grad_hidden = grad_top.astype(F32) + norm_backward_step(
        grad_normed_two, hat_two, inverse_two, gain_mlp
    )
    expert_out = mm_nt(inner_bf, full_down).astype(BF).astype(F32)
    weighted = coef * expert_out
    weighted = weighted.astype(BF)
    route_part = jnp.sum(grad_all.astype(F32) * expert_out, -1)
    grad_hidden_bf = after(grad_hidden.astype(BF), grad_w_experts)
    grad_att = collect_crossed(grad_hidden_bf, "shard")
    grad_att, weighted = lax.optimization_barrier((grad_att, weighted))
    mixture = reduce_blocks(block_rows_of(weighted), False)
    block_out = (hidden + mixture).astype(BF)
    route_all = {0: route_part[:own_rows]}
    for k in order_of(count_s):
        route_all[k] = swap(route_part[k * own_rows : (k + 1) * own_rows], "shard", k)
    route_grad = jnp.zeros(ids.shape, F32)
    for k in range(count_s):
        route_grad = jnp.where(ids == (me_s ^ k), route_all[k][:, None], route_grad)

    attention_gradient = mm(grad_att, full_out).astype(BF)

    grad_q, grad_kv, gain_q_parts = pl.pallas_call(
        attn_grad_kernel,
        grid_spec=pltpu.PrefetchScalarGridSpec(
            num_scalar_prefetch=1,
            grid=(seqs,),
            in_specs=[
                nat_spec, row_spec, kv_spec, row_spec, row_spec, lse_spec,
                gain_spec, table_spec, table_spec,
            ],
            out_specs=[row_spec, kv_spec, pl.BlockSpec((1, 1, head_dim), lambda s, _: (s, 0, 0))],
            scratch_shapes=[
                pltpu.VMEM((block_rows, q_width), F32),
                pltpu.VMEM((seq_len, head_dim), BF),
                pltpu.VMEM((seq_len, head_dim), BF),
                pltpu.VMEM((block_rows, q_width), BF),
                pltpu.VMEM((block_rows, q_width), BF),
                pltpu.VMEM((seq_len, head_dim), F32),
                pltpu.VMEM((seq_len, head_dim), F32),
            ],
        ),
        out_shape=[
            jax.ShapeDtypeStruct((count_s, seqs, own, q_width), BF),
            jax.ShapeDtypeStruct((count_c, 2, count_s, seqs, own, head_dim), BF),
            jax.ShapeDtypeStruct((seqs, 1, head_dim), F32),
        ],
        name="attn_bwd",
        cost_estimate=pl.CostEstimate(
            flops=10 * all_rows * seq_len * q_width, bytes_accessed=32 * all_rows * q_width, transcendentals=0
        ),
    )(
        me_ids, queries_bf, queries, kv_all,
        attention_gradient.reshape(count_s, seqs, own, q_width),
        attn, lse, gain_q_row, cos_nat, sin_nat,
    )
    grad_kv = grad_kv.reshape(count_c, 2, all_rows, head_dim)
    grad_q = grad_q.reshape(all_rows, q_width)
    grad_w_query = mm_tn(normed_one, grad_q).astype(BF)
    sum_query = scatter(grad_w_query).astype(F32)
    query_part = reduce_blocks(
        lambda k, columns: mm_nt(grad_q[k * own_rows : (k + 1) * own_rows], full_query[columns]),
        False,
    )
    grad_w_out = mm_tn(after(grad_att, grad_kv), attn.reshape(all_rows, q_width)).astype(BF)
    half_sum_out = sum_cores(grad_w_out)

    kv_parts = [grad_kv[0]]
    for k in range(1, count_c):
        kv_parts.append(swap(grad_kv[k], "ctx", k))
    kv_parts = list(lax.optimization_barrier((*kv_parts, half_sum_out))[:count_c])
    grad_kv_bf, gain_k_part = pl.pallas_call(
        functools.partial(key_grad_kernel, count_c),
        out_shape=[
            jax.ShapeDtypeStruct((all_rows, 2 * head_dim), BF),
            jax.ShapeDtypeStruct((1, head_dim), F32),
        ],
        name="key_grad",
    )(kv_raw, gain_k_row, cos_rows, sin_rows, *kv_parts)
    kv_rows = {
        k: swap(grad_kv_bf[k * own_rows : (k + 1) * own_rows], "shard", k)
        for k in order_of(count_s)
    }
    kv_rows[0] = grad_kv_bf[:own_rows]
    half_sum_kv = sum_cores(mm_tn(normed_one, grad_kv_bf).astype(BF))
    sum_kv = sum_ctx(half_sum_kv, sum_query)
    kv_all_rows = jnp.concatenate([kv_rows[k] for k in range(count_s)], 1)
    expert_parts = jnp.split(sum_experts[None], 3, 2)
    kv_all_rows, _, *expert_parts = lax.optimization_barrier(
        (kv_all_rows, half_sum_kv, *expert_parts)
    )
    grad_normed_one = query_part + mm_nt(kv_all_rows, kv_weights)
    gain_attn_part = jnp.sum(grad_normed_one * hat_own, 0)
    grad_tokens = grad_hidden + norm_backward_step(
        grad_normed_one, hat_own, inverse_own, gain_attn
    )
    gains = jnp.concatenate(
        [gain_attn_part, gain_mlp_part, jnp.sum(gain_q_parts, (0, 1)), gain_k_part[0]]
    ).reshape(-1, head_dim)
    for axis in ("dp", "shard", "ctx"):
        step = 1
        while step < lax.axis_size(axis):
            gains = gains + swap(gains, axis, step)
            step *= 2
        if axis == "shard":
            sum_out = sum_ctx(half_sum_out, gains)
    gains = gains.reshape(-1)

    def own_shape(value):
        return value.reshape(seqs, own, value.shape[-1])

    return (
        own_shape(block_out),
        own_shape(grad_tokens),
        lse,
        own_shape(route_grad),
        gains[:width],
        gains[width : 2 * width],
        gains[2 * width : 2 * width + head_dim],
        gains[2 * width + head_dim :],
        sum_query,
        sum_kv[:, :head_dim],
        sum_kv[:, head_dim:],
        sum_out,
        *expert_parts,
    )


def solution(mesh):
    placed = (
        P("dp", "ctx", None),
        P(),
        P(),
        P(),
        P(),
        P(("ctx", "dp"), "shard"),
        P(("ctx", "dp"), "shard"),
        P(("ctx", "dp"), "shard"),
        P(("ctx", "dp"), "shard"),
        P("shard", ("ctx", "dp"), None),
        P("shard", ("ctx", "dp"), None),
        P("shard", ("ctx", "dp"), None),
        P("dp", ("ctx", "shard"), None),
        P("dp", ("ctx", "shard"), None),
        P("dp", ("ctx", "shard"), None),
    )

    return jax.shard_map(
        per_device,
        mesh=mesh,
        in_specs=placed,
        out_specs=(
            P("dp", ("ctx", "shard"), None),
            P("dp", ("ctx", "shard"), None),
            P("dp", "shard", "ctx"),
            P("dp", ("ctx", "shard"), None),
            P(),
            P(),
            P(),
            P(),
            P(("ctx", "dp"), "shard"),
            P(("ctx", "dp"), "shard"),
            P(("ctx", "dp"), "shard"),
            P(("ctx", "dp"), "shard"),
            P("shard", ("ctx", "dp"), None),
            P("shard", ("ctx", "dp"), None),
            P("shard", ("ctx", "dp"), None),
        ),
        check_vma=False,
    )
```

```python
import functools

import jax
import jax.numpy as jnp
from jax import lax
from jax.experimental import pallas as pl
from jax.experimental.pallas import tpu as pltpu
from jax.sharding import PartitionSpec as P


epsilon = 1e-06
theta_base = 1000000.0
BF = jnp.bfloat16
F32 = jnp.float32


def pairs(count, k):
    return [(i, i ^ k) for i in range(count)]


def swap(value, axis, k):
    return lax.ppermute(value, axis, pairs(lax.axis_size(axis), k))


def order_of(count):
    return sorted(range(1, count), key=lambda k: -bin(k).count("1"))


def collect(value, axis):
    count = lax.axis_size(axis)
    got = {0: value}
    for k in order_of(count):
        got[k] = swap(value, axis, k)
    return [got[k] for k in range(count)]


def join_kernel(*refs):
    *parts, out_ref = refs
    rows, half = parts[0].shape
    for k in range(len(parts) // 2):
        out_ref[k * rows : (k + 1) * rows, :half] = parts[2 * k][...]
        out_ref[k * rows : (k + 1) * rows, half:] = parts[2 * k + 1][...]


def join(parts):
    rows, half = parts[0].shape
    shape = (len(parts) // 2 * rows, 2 * half)
    return pl.pallas_call(
        join_kernel,
        out_shape=jax.ShapeDtypeStruct(shape, parts[0].dtype),
        name="join",
        cost_estimate=pl.CostEstimate(
            flops=0, bytes_accessed=4 * shape[0] * shape[1], transcendentals=0
        ),
    )(*parts)


def collect_crossed(value, axis, *others):
    if lax.axis_size(axis) != 4:
        return after(jnp.concatenate(collect(value, axis), 0), *others), ()
    half = value.shape[1] // 2
    low, high = value[:, :half], value[:, half:]

    def send(part, k):
        return swap(part, axis, k)

    low_1, high_2 = send(low, 1), send(high, 2)
    high_1, low_2 = send(high, 1), send(low, 2)
    low_3, high_3 = send(low_1, 2), send(high_2, 1)
    parts = (low, high, low_1, high_1, low_2, high_2, low_3, high_3)
    return join(lax.optimization_barrier((*parts, *others))[: len(parts)]), (low_1, high_2)


def folded_positions(rows, count_ctx, half_block):
    block = rows // half_block
    offset = rows % half_block
    device = block // 2
    placed = jnp.where(block % 2 == 0, device, 2 * count_ctx - 1 - device)
    return placed * half_block + offset


def rope_tables(positions, head_dim):
    freq = jnp.arange(head_dim // 2, dtype=F32) * (2.0 / head_dim)
    inverse = jnp.power(jnp.float32(theta_base), -freq)
    angles = positions.astype(F32)[..., None] * inverse
    cosine, sine = jnp.cos(angles), jnp.sin(angles)
    return jnp.concatenate([cosine, cosine], -1), jnp.concatenate([-sine, sine], -1)


def inv_rms(field):
    return lax.rsqrt(jnp.mean(field * field, -1, keepdims=True) + epsilon)


def norm_backward_step(grad_normed, normed_hat, inverse, gain):
    scaled = grad_normed * gain
    return inverse * (scaled - normed_hat * jnp.mean(scaled * normed_hat, -1, keepdims=True))


def mm(a, b):
    return lax.dot_general(a, b, (((1,), (0,)), ((), ())), preferred_element_type=F32)


def mm_nt(a, b):
    return lax.dot_general(a, b, (((1,), (1,)), ((), ())), preferred_element_type=F32)


def mm_tn(a, b):
    return lax.dot_general(a, b, (((0,), (0,)), ((), ())), preferred_element_type=F32)


def turn(u, cosine, sine):
    return u * cosine + pltpu.roll(u, u.shape[-1] // 2, 1) * sine


def turn_back(u, cosine, sine):
    return u * cosine - pltpu.roll(u, u.shape[-1] // 2, 1) * sine


def key_kernel(raw_ref, gain_ref, cos_ref, sin_ref, out_ref):
    dim = gain_ref.shape[-1]
    raw = raw_ref[:, :dim]
    unit = raw * inv_rms(raw)
    out_ref[0] = turn(unit * gain_ref[...], cos_ref[...], sin_ref[...]).astype(BF)
    out_ref[1] = raw_ref[:, dim:].astype(BF)


def key_grad_kernel(count, raw_ref, gain_ref, cos_ref, sin_ref, *refs):
    parts, (out_ref, gain_out) = refs[:count], refs[count:]
    dim = gain_ref.shape[-1]
    total = parts[0][...].astype(F32)
    for part in parts[1:]:
        total = total + part[...].astype(F32)
    raw = raw_ref[:, :dim]
    inverse = inv_rms(raw)
    unit = raw * inverse
    grad = turn_back(total[0], cos_ref[...], sin_ref[...])
    gain_out[...] = jnp.sum(grad * unit, 0, keepdims=True)
    out_ref[:, :dim] = norm_backward_step(grad, unit, inverse, gain_ref[...]).astype(BF)
    out_ref[:, dim:] = total[1].astype(BF)


def natural_rows(me_s, count_s, ref, out_ref):
    own = out_ref.shape[0] // count_s
    for j in range(count_s):
        out_ref[j * own : (j + 1) * own, :] = ref[me_s ^ j, 0]


def gather_keys(me_s, me_c, kv_ref, k_nat, v_nat):
    count_c, _, count_s, _, own, _ = kv_ref.shape
    half = count_s * own // 2
    for jc in range(count_c):
        for j in range(count_s):
            row = j * own
            at = jc * half + row if row < half else (2 * count_c - 1 - jc) * half + row - half
            k_nat[at : at + own, :] = kv_ref[me_c ^ jc, 0, me_s ^ j, 0]
            v_nat[at : at + own, :] = kv_ref[me_c ^ jc, 1, me_s ^ j, 0]


def masks(me_c, count_c, half):
    length = count_c * half
    key = lax.broadcasted_iota(jnp.int32, (length, half), 0)
    lane = lax.broadcasted_iota(jnp.int32, (length, half), 1)
    near = key <= me_c * half + lane
    far = key + length <= (2 * count_c - 1 - me_c) * half + lane
    return near, far


def attn_kernel(ids_ref, q_ref, kv_ref, gain_ref, cos_ref, sin_ref, attn_ref, lse_ref, qb_ref, q_nat, k_nat, v_nat):
    me_s, me_c = ids_ref[0], ids_ref[1]
    count_s, _, own, width = q_ref.shape
    count_c = kv_ref.shape[0]
    dim = gain_ref.shape[-1]
    rows = count_s * own
    half = rows // 2
    length = count_c * half
    scale = dim ** (-0.5)
    natural_rows(me_s, count_s, q_ref, q_nat)
    gather_keys(me_s, me_c, kv_ref, k_nat, v_nat)
    near, far = masks(me_c, count_c, half)
    v_t = v_nat[...].astype(F32).T.astype(BF)
    for h in range(width // dim):
        lanes = slice(h * dim, (h + 1) * dim)
        u = q_nat[:, lanes]
        q = turn(u * inv_rms(u) * gain_ref[...], cos_ref[...], sin_ref[...]).astype(BF)
        qb_ref[0, :, lanes] = q
        s_a = mm_nt(k_nat[:length], q) * scale
        s_n = jnp.where(near, s_a[:, :half], -1e30)
        s_f = s_a[:, half:]
        s_b = jnp.where(far, mm_nt(k_nat[length:], q[half:]) * scale, -1e30)
        m_n = jnp.max(s_n, 0, keepdims=True)
        m_f = jnp.maximum(jnp.max(s_f, 0, keepdims=True), jnp.max(s_b, 0, keepdims=True))
        e_n = jnp.exp(s_n - m_n)
        e_f = jnp.exp(s_f - m_f)
        e_b = jnp.exp(s_b - m_f)
        l_n = jnp.sum(e_n, 0, keepdims=True)
        l_f = jnp.sum(e_f, 0, keepdims=True) + jnp.sum(e_b, 0, keepdims=True)
        lse_ref[0, h : h + 1, :half] = m_n + jnp.log(l_n)
        lse_ref[0, h : h + 1, half:] = m_f + jnp.log(l_f)
        r_n, r_f = 1.0 / l_n, 1.0 / l_f
        o_n = mm(v_t[:, :length], (e_n * r_n).astype(BF))
        o_f = mm(v_t[:, :length], (e_f * r_f).astype(BF)) + mm(v_t[:, length:], (e_b * r_f).astype(BF))
        o = jnp.concatenate([o_n.T, o_f.T], 0).astype(BF)
        for j in range(count_s):
            attn_ref[me_s ^ j, 0, :, lanes] = o[j * own : (j + 1) * own]


def attn_grad_kernel(ids_ref, qb_ref, q_ref, kv_ref, do_ref, attn_ref, lse_ref, gain_ref, cos_ref, sin_ref, gq_ref, dkv_ref, gain_out, q_nat, k_nat, v_nat, do_nat, attn_nat, dk_acc, dv_acc):
    me_s, me_c = ids_ref[0], ids_ref[1]
    count_s, _, own, width = q_ref.shape
    count_c = kv_ref.shape[0]
    dim = gain_ref.shape[-1]
    rows = count_s * own
    half = rows // 2
    length = count_c * half
    scale = dim ** (-0.5)
    natural_rows(me_s, count_s, q_ref, q_nat)
    natural_rows(me_s, count_s, do_ref, do_nat)
    natural_rows(me_s, count_s, attn_ref, attn_nat)
    gather_keys(me_s, me_c, kv_ref, k_nat, v_nat)
    near, far = masks(me_c, count_c, half)
    k_t = k_nat[...].astype(F32).T.astype(BF)
    heads = width // dim
    lane = lax.broadcasted_iota(jnp.int32, (rows, dim), 1)
    delta = jnp.zeros((rows, dim), F32)
    for h in range(heads):
        lanes = slice(h * dim, (h + 1) * dim)
        both = jnp.sum(do_nat[:, lanes].astype(F32) * attn_nat[:, lanes].astype(F32), -1, keepdims=True)
        delta = jnp.where(lane == h, both, delta)
    delta_t = delta.T
    gain_total = jnp.zeros((1, dim), F32)
    for h in range(heads):
        lanes = slice(h * dim, (h + 1) * dim)
        q = qb_ref[0, :, lanes]
        do = do_nat[:, lanes]
        lse = lse_ref[0, h : h + 1, :]
        dlt = delta_t[h : h + 1, :]
        s_a = mm_nt(k_nat[:length], q) * scale
        dp_a = mm_nt(v_nat[:length], do)
        p_n = jnp.exp(jnp.where(near, s_a[:, :half], -1e30) - lse[:, :half])
        p_f = jnp.exp(s_a[:, half:] - lse[:, half:])
        p_a = jnp.concatenate([p_n, p_f], 1)
        ds_a = (p_a * (dp_a - dlt) * scale).astype(BF)
        p_a = p_a.astype(BF)
        s_b = jnp.where(far, mm_nt(k_nat[length:], q[half:]) * scale, -1e30)
        dp_b = mm_nt(v_nat[length:], do[half:])
        p_b = jnp.exp(s_b - lse[:, half:])
        ds_b = (p_b * (dp_b - dlt[:, half:]) * scale).astype(BF)
        p_b = p_b.astype(BF)
        dk_a, dv_a = mm(ds_a, q), mm(p_a, do)
        dk_b, dv_b = mm(ds_b, q[half:]), mm(p_b, do[half:])
        if h == 0:
            dk_acc[:length], dv_acc[:length] = dk_a, dv_a
            dk_acc[length:], dv_acc[length:] = dk_b, dv_b
        else:
            dk_acc[:length] += dk_a
            dv_acc[:length] += dv_a
            dk_acc[length:] += dk_b
            dv_acc[length:] += dv_b
        dq_a = mm(k_t[:, :length], ds_a)
        dq_f = dq_a[:, half:] + mm(k_t[:, length:], ds_b)
        dq = jnp.concatenate([dq_a[:, :half].T, dq_f.T], 0)
        grad = turn_back(dq, cos_ref[...], sin_ref[...])
        u = q_nat[:, lanes]
        inverse = inv_rms(u)
        hat = u * inverse
        gain_total = gain_total + jnp.sum(grad * hat, 0, keepdims=True)
        out = norm_backward_step(grad, hat, inverse, gain_ref[...]).astype(BF)
        for j in range(count_s):
            gq_ref[me_s ^ j, 0, :, lanes] = out[j * own : (j + 1) * own]
    gain_out[0] = gain_total
    for jc in range(count_c):
        for j in range(count_s):
            row = j * own
            at = jc * half + row if row < half else (2 * count_c - 1 - jc) * half + row - half
            dkv_ref[me_c ^ jc, 0, me_s ^ j, 0] = dk_acc[at : at + own, :].astype(BF)
            dkv_ref[me_c ^ jc, 1, me_s ^ j, 0] = dv_acc[at : at + own, :].astype(BF)


def expert_grad_kernel(rows_ref, grad_in_ref, grads_ref, inner_ref, out_ref):
    wide = grads_ref.shape[1]
    out_ref[:, :wide] = mm_tn(rows_ref[...], grads_ref[...]).astype(BF)
    out_ref[:, wide:] = mm_tn(grad_in_ref[...], inner_ref[...]).astype(BF)


def expert_grads(rows, grad_in, grads, inner):
    count, width = rows.shape
    tile = 256 if width % 256 == 0 else width
    wide = grads.shape[1] + inner.shape[1]

    def resident(value):
        return pl.BlockSpec(value.shape, lambda i: (0, 0))

    return pl.pallas_call(
        expert_grad_kernel,
        grid=(width // tile,),
        in_specs=[
            pl.BlockSpec((count, tile), lambda i: (0, i)),
            pl.BlockSpec((count, tile), lambda i: (0, i)),
            resident(grads),
            resident(inner),
        ],
        out_specs=pl.BlockSpec((tile, wide), lambda i: (i, 0)),
        out_shape=jax.ShapeDtypeStruct((width, wide), BF),
        name="expert_grads",
        cost_estimate=pl.CostEstimate(
            flops=2 * count * width * wide, bytes_accessed=4 * (count + wide) * width, transcendentals=0
        ),
    )(rows, grad_in, grads, inner)


def after(value, *others):
    return lax.optimization_barrier((value, *others))[0]


def per_device(
    tokens,
    gain_attn,
    gain_mlp,
    gain_query,
    key_norm_gain,
    w_query,
    key_matrix,
    value_matrix,
    w_out,
    w_gate,
    w_up,
    w_down,
    expert_ids,
    route_weight,
    cotangent,
):
    count_c = lax.axis_size("ctx")
    count_s = lax.axis_size("shard")
    me_c = lax.axis_index("ctx")
    me_s = lax.axis_index("shard")
    seqs, block_rows, width = tokens.shape
    own = expert_ids.shape[1]
    head_dim = gain_query.shape[0]
    q_width = w_query.shape[1]
    heads = q_width // head_dim
    hidden_width = w_gate.shape[2]
    half = block_rows // 2
    seq_len = block_rows * count_c
    own_rows = seqs * own
    all_rows = count_s * own_rows
    both = ("ctx", "dp")

    def gather(value):
        return lax.all_gather(value, both, axis=0, tiled=True)

    def scatter(value):
        return lax.psum_scatter(value, both, scatter_dimension=0, tiled=True)

    def sum_cores(value):
        count_d = lax.axis_size("dp")
        me_d = lax.axis_index("dp")
        parts = value.reshape(count_c, count_d, -1, value.shape[1])
        total = lax.dynamic_index_in_dim(parts, me_d, 1, False).astype(F32)
        for k in range(1, count_d):
            sent = lax.dynamic_index_in_dim(parts, me_d ^ k, 1, False)
            total = total + swap(sent, "dp", k).astype(F32)
        return total.astype(BF)

    def sum_ctx(total, *others):
        result = lax.dynamic_index_in_dim(total, me_c, 0, False).astype(F32)
        parts = []
        for k in order_of(count_c):
            sent = lax.dynamic_index_in_dim(total, me_c ^ k, 0, False)
            parts.append(swap(sent, "ctx", k))
        parts = lax.optimization_barrier((*parts, *others))[: len(parts)]
        for part in parts:
            result = result + part.astype(F32)
        return result

    full_qkv = gather(jnp.concatenate([w_query, key_matrix, value_matrix], 1))
    full_out = gather(w_out)
    full_experts = gather(jnp.concatenate([w_gate[0], w_up[0], w_down[0]], 1))

    rows_at = [
        lax.dynamic_slice_in_dim(tokens, (me_s ^ k) * own, own, 1).reshape(own_rows, width)
        for k in range(count_s)
    ]
    residual = jnp.concatenate(rows_at, 0).astype(F32)
    inverse_one = inv_rms(residual)
    hat_one = residual * inverse_one
    normed_one = (hat_one * gain_attn).astype(BF)
    residual_own = rows_at[0].astype(F32)
    inverse_own = inv_rms(residual_own)
    hat_own = residual_own * inverse_own

    grad_top = cotangent.reshape(own_rows, width)
    grad_all = jnp.concatenate(collect(grad_top, "shard"), 0)
    ids = expert_ids.reshape(own_rows, -1)
    weights = route_weight.reshape(own_rows, -1)

    def weight_for(expert):
        return jnp.sum(jnp.where(ids == expert, weights, 0.0), -1)

    coefs = {0: weight_for(me_s)}
    for k in order_of(count_s):
        coefs[k] = swap(weight_for(me_s ^ k), "shard", k)
    coef = jnp.concatenate([coefs[k] for k in range(count_s)], 0)[:, None]
    grad_rows = (coef * grad_all.astype(F32)).astype(BF)

    block = jnp.arange(count_s, dtype=jnp.int32)
    offsets = jnp.arange(own, dtype=jnp.int32)
    row_natural = me_c * block_rows + jnp.arange(block_rows, dtype=jnp.int32)
    cos_nat, sin_nat = rope_tables(folded_positions(row_natural, count_c, half), head_dim)
    row_peer = me_c * block_rows + (me_s ^ block)[:, None] * own + offsets
    cos_peer, sin_peer = rope_tables(folded_positions(row_peer, count_c, half), head_dim)

    def spread(table):
        return jnp.broadcast_to(
            table[:, None], (count_s, seqs, own, head_dim)
        ).reshape(all_rows, head_dim)

    cos_rows, sin_rows = spread(cos_peer), spread(sin_peer)
    gain_q_row, gain_k_row = gain_query[None], key_norm_gain[None]

    normed_one = after(normed_one, grad_rows)
    kv_raw = mm(normed_one, full_qkv[:, q_width:])
    kv_own = pl.pallas_call(
        key_kernel, out_shape=jax.ShapeDtypeStruct((2, all_rows, head_dim), BF), name="key_prep"
    )(kv_raw, gain_k_row, cos_rows, sin_rows)
    kv_all = jnp.stack(collect(kv_own, "ctx"), 0).reshape(
        count_c, 2, count_s, seqs, own, head_dim
    )
    full_query = lax.optimization_barrier(full_qkv[:, :q_width])
    queries = mm(normed_one, full_query).reshape(count_s, seqs, own, q_width)
    kv_weights = [full_qkv[:, q_width:]]
    for k in range(1, count_s):
        kv_weights.append(swap(kv_weights[0], "shard", k))
    kv_weights = jnp.concatenate(kv_weights, 1)

    me_ids = jnp.stack([me_s, me_c]).astype(jnp.int32)
    row_spec = pl.BlockSpec((count_s, 1, own, q_width), lambda s, _: (0, s, 0, 0))
    kv_spec = pl.BlockSpec(
        (count_c, 2, count_s, 1, own, head_dim), lambda s, _: (0, 0, 0, s, 0, 0)
    )
    nat_spec = pl.BlockSpec((1, block_rows, q_width), lambda s, _: (s, 0, 0))
    lse_spec = pl.BlockSpec((1, heads, block_rows), lambda s, _: (s, 0, 0))

    def whole(shape):
        return pl.BlockSpec(shape, lambda s, _: (0,) * len(shape))

    table_spec = whole((block_rows, head_dim))
    gain_spec = whole((1, head_dim))
    attn, lse, queries_bf = pl.pallas_call(
        attn_kernel,
        grid_spec=pltpu.PrefetchScalarGridSpec(
            num_scalar_prefetch=1,
            grid=(seqs,),
            in_specs=[row_spec, kv_spec, gain_spec, table_spec, table_spec],
            out_specs=[row_spec, lse_spec, nat_spec],
            scratch_shapes=[
                pltpu.VMEM((block_rows, q_width), F32),
                pltpu.VMEM((seq_len, head_dim), BF),
                pltpu.VMEM((seq_len, head_dim), BF),
            ],
        ),
        out_shape=[
            jax.ShapeDtypeStruct((count_s, seqs, own, q_width), BF),
            jax.ShapeDtypeStruct((seqs, heads, block_rows), F32),
            jax.ShapeDtypeStruct((seqs, block_rows, q_width), BF),
        ],
        name="attn_fwd",
        cost_estimate=pl.CostEstimate(
            flops=4 * all_rows * seq_len * q_width, bytes_accessed=16 * all_rows * q_width, transcendentals=0
        ),
    )(me_ids, queries, kv_all, gain_q_row, cos_nat, sin_nat)

    half_width = width // 2
    sides = (slice(0, half_width), slice(half_width, width))

    def reduce_blocks(term, crossed):
        def send(value, k):
            return swap(value.astype(BF), "shard", k)

        low, high = sides
        if count_s != 4 or not crossed:
            full = slice(0, width)
            got = {k: send(term(k, full), k) for k in order_of(count_s)}
            total = term(0, full).astype(F32)
            for part in got.values():
                total = total + part.astype(F32)
            return total
        far_low = send(term(3, low), 1)
        far_high = send(term(3, high), 2)
        near_low = send(term(1, low), 1)
        near_high = send(term(2, high), 2)
        relay_low = swap((term(2, low).astype(F32) + far_low.astype(F32)).astype(BF), "shard", 2)
        relay_high = swap((term(1, high).astype(F32) + far_high.astype(F32)).astype(BF), "shard", 1)
        total_low = term(0, low).astype(F32) + near_low.astype(F32) + relay_low.astype(F32)
        total_high = term(0, high).astype(F32) + near_high.astype(F32) + relay_high.astype(F32)
        return jnp.concatenate([total_low, total_high], 1)

    def block_rows_of(value):
        return lambda k, columns: value[k * own_rows : (k + 1) * own_rows, columns]

    attended = reduce_blocks(
        lambda k, columns: mm_nt(attn[k].reshape(own_rows, q_width), full_out[columns]), True
    )
    hidden = residual_own + attended
    inverse_two = inv_rms(hidden)
    hat_two = hidden * inverse_two
    normed_two = (hat_two * gain_mlp).astype(BF)
    arrived, _ = collect_crossed(normed_two, "shard", kv_weights)

    full_gate_up = full_experts[:, : 2 * hidden_width]
    full_down = full_experts[:, 2 * hidden_width :]
    grad_inner = mm(grad_rows, full_down)
    pre = mm(arrived, full_gate_up)
    gate_pre, up_pre = pre[:, :hidden_width], pre[:, hidden_width:]
    gate_sig = jax.nn.sigmoid(gate_pre)
    gate_act = gate_pre * gate_sig
    inner_bf = (gate_act * up_pre).astype(BF)
    grad_gate = grad_inner * up_pre * gate_sig * (1.0 + gate_pre * (1.0 - gate_sig))
    grad_up = grad_inner * gate_act
    grad_gate_up = jnp.concatenate([grad_gate.astype(BF), grad_up.astype(BF)], 1)
    grad_slots = mm_nt(grad_gate_up, full_gate_up)
    grad_normed_two = reduce_blocks(block_rows_of(grad_slots.astype(BF)), True)
    grad_w_experts = expert_grads(arrived, grad_rows, after(grad_gate_up, grad_slots), inner_bf)
    sum_experts = scatter(grad_w_experts).astype(F32)

    gain_mlp_part = jnp.sum(grad_normed_two * hat_two, 0)
    grad_hidden = grad_top.astype(F32) + norm_backward_step(
        grad_normed_two, hat_two, inverse_two, gain_mlp
    )
    grad_hidden_bf = after(grad_hidden.astype(BF), grad_w_experts)
    grad_att, first_in = collect_crossed(grad_hidden_bf, "shard")
    expert_out = mm_nt(after(inner_bf, *first_in), full_down).astype(BF).astype(F32)
    weighted = coef * expert_out
    weighted = weighted.astype(BF)
    route_part = jnp.sum(grad_all.astype(F32) * expert_out, -1)
    weighted = [weighted[k * own_rows : (k + 1) * own_rows] for k in range(count_s)]
    grad_att, *weighted = lax.optimization_barrier((grad_att, *weighted))
    mixture = reduce_blocks(lambda k, columns: weighted[k], False)
    block_out = (hidden + mixture).astype(BF)
    attention_gradient = mm(grad_att, full_out).astype(BF)

    grad_q, grad_kv, gain_q_parts = pl.pallas_call(
        attn_grad_kernel,
        grid_spec=pltpu.PrefetchScalarGridSpec(
            num_scalar_prefetch=1,
            grid=(seqs,),
            in_specs=[
                nat_spec, row_spec, kv_spec, row_spec, row_spec, lse_spec,
                gain_spec, table_spec, table_spec,
            ],
            out_specs=[row_spec, kv_spec, pl.BlockSpec((1, 1, head_dim), lambda s, _: (s, 0, 0))],
            scratch_shapes=[
                pltpu.VMEM((block_rows, q_width), F32),
                pltpu.VMEM((seq_len, head_dim), BF),
                pltpu.VMEM((seq_len, head_dim), BF),
                pltpu.VMEM((block_rows, q_width), BF),
                pltpu.VMEM((block_rows, q_width), BF),
                pltpu.VMEM((seq_len, head_dim), F32),
                pltpu.VMEM((seq_len, head_dim), F32),
            ],
        ),
        out_shape=[
            jax.ShapeDtypeStruct((count_s, seqs, own, q_width), BF),
            jax.ShapeDtypeStruct((count_c, 2, count_s, seqs, own, head_dim), BF),
            jax.ShapeDtypeStruct((seqs, 1, head_dim), F32),
        ],
        name="attn_bwd",
        cost_estimate=pl.CostEstimate(
            flops=10 * all_rows * seq_len * q_width, bytes_accessed=32 * all_rows * q_width, transcendentals=0
        ),
    )(
        me_ids, queries_bf, queries, kv_all,
        attention_gradient.reshape(count_s, seqs, own, q_width),
        attn, lse, gain_q_row, cos_nat, sin_nat,
    )
    grad_kv = grad_kv.reshape(count_c, 2, all_rows, head_dim)
    grad_q = grad_q.reshape(all_rows, q_width)
    grad_w_query = mm_tn(normed_one, grad_q).astype(BF)
    sum_query = scatter(grad_w_query)

    def query_term(k, columns):
        return mm_nt(grad_q[k * own_rows : (k + 1) * own_rows], full_query[columns])

    query_part = reduce_blocks(query_term, False)

    grad_w_out = mm_tn(after(grad_att, grad_kv), attn.reshape(all_rows, q_width)).astype(BF)
    half_sum_out = sum_cores(grad_w_out)
    kv_parts = [grad_kv[0]]
    for k in range(1, count_c):
        kv_parts.append(swap(grad_kv[k], "ctx", k))
    kv_parts = list(lax.optimization_barrier((*kv_parts, half_sum_out))[:count_c])
    grad_kv_bf, gain_k_part = pl.pallas_call(
        functools.partial(key_grad_kernel, count_c),
        out_shape=[
            jax.ShapeDtypeStruct((all_rows, 2 * head_dim), BF),
            jax.ShapeDtypeStruct((1, head_dim), F32),
        ],
        name="key_grad",
    )(kv_raw, gain_k_row, cos_rows, sin_rows, *kv_parts)
    kv_rows = {
        k: swap(grad_kv_bf[k * own_rows : (k + 1) * own_rows], "shard", k)
        for k in order_of(count_s)
    }
    kv_rows[0] = grad_kv_bf[:own_rows]
    half_sum_kv = sum_cores(mm_tn(normed_one, grad_kv_bf).astype(BF))
    kv_all_rows = jnp.concatenate([kv_rows[k] for k in range(count_s)], 1)
    expert_parts = jnp.split(sum_experts[None], 3, 2)
    kv_all_rows, _, *expert_parts = lax.optimization_barrier(
        (kv_all_rows, half_sum_kv, *expert_parts)
    )
    grad_normed_one = query_part + mm_nt(kv_all_rows, kv_weights)
    gain_attn_part = jnp.sum(grad_normed_one * hat_own, 0)
    route_part = after(route_part, gain_attn_part)
    route_all = {0: route_part[:own_rows]}
    for k in order_of(count_s):
        route_all[k] = swap(route_part[k * own_rows : (k + 1) * own_rows], "shard", k)
    route_grad = jnp.zeros(ids.shape, F32)
    for k in range(count_s):
        route_grad = jnp.where(ids == (me_s ^ k), route_all[k][:, None], route_grad)

    grad_tokens = grad_hidden + norm_backward_step(
        grad_normed_one, hat_own, inverse_own, gain_attn
    )
    gains = jnp.concatenate(
        [gain_attn_part, gain_mlp_part, jnp.sum(gain_q_parts, (0, 1)), gain_k_part[0]]
    ).reshape(-1, head_dim)
    for axis in ("dp", "shard", "ctx"):
        terms = collect(gains, axis)
        while len(terms) > 1:
            terms = [one + other for one, other in zip(terms[::2], terms[1::2])]
        gains = terms[0]
        if axis == "shard":
            sum_out = sum_ctx(half_sum_out, gains)
            sum_kv = sum_ctx(half_sum_kv, gains)
            sum_query = after(sum_query, gains).astype(F32)
    gains = gains.reshape(-1)

    def own_shape(value):
        return value.reshape(seqs, own, value.shape[-1])

    return (
        own_shape(block_out),
        own_shape(grad_tokens),
        lse,
        own_shape(route_grad),
        gains[:width],
        gains[width : 2 * width],
        gains[2 * width : 2 * width + head_dim],
        gains[2 * width + head_dim :],
        sum_query,
        sum_kv[:, :head_dim],
        sum_kv[:, head_dim:],
        sum_out,
        *expert_parts,
    )


def solution(mesh):
    placed = (
        P("dp", "ctx", None),
        P(),
        P(),
        P(),
        P(),
        P(("ctx", "dp"), "shard"),
        P(("ctx", "dp"), "shard"),
        P(("ctx", "dp"), "shard"),
        P(("ctx", "dp"), "shard"),
        P("shard", ("ctx", "dp"), None),
        P("shard", ("ctx", "dp"), None),
        P("shard", ("ctx", "dp"), None),
        P("dp", ("ctx", "shard"), None),
        P("dp", ("ctx", "shard"), None),
        P("dp", ("ctx", "shard"), None),
    )

    return jax.shard_map(
        per_device,
        mesh=mesh,
        in_specs=placed,
        out_specs=(
            P("dp", ("ctx", "shard"), None),
            P("dp", ("ctx", "shard"), None),
            P("dp", "shard", "ctx"),
            P("dp", ("ctx", "shard"), None),
            P(),
            P(),
            P(),
            P(),
            P(("ctx", "dp"), "shard"),
            P(("ctx", "dp"), "shard"),
            P(("ctx", "dp"), "shard"),
            P(("ctx", "dp"), "shard"),
            P("shard", ("ctx", "dp"), None),
            P("shard", ("ctx", "dp"), None),
            P("shard", ("ctx", "dp"), None),
        ),
        check_vma=False,
    )
```
